16 devices in a mesh: dp: 4 (over z, y), ep: 4 (over x, core).
Axes of the slice: x: 2, y: 2, z: 2, core: 2. Of those that a mesh axis runs over, the one named last changes fastest.
Arguments:
- tokens_a: bfloat16 [512, 1536], P(('dp', 'ep')), parts along dimension 0
- experts_a: int32 [512, 8], P(('dp', 'ep')), parts along dimension 0
- slots_a: int32 [512, 8], P(('dp', 'ep')), parts along dimension 0
- gates_a: bfloat16 [512, 8], P(('dp', 'ep')), parts along dimension 0
- tokens_b: bfloat16 [512, 1536], P(('dp', 'ep')), parts along dimension 0
- experts_b: int32 [512, 8], P(('dp', 'ep')), parts along dimension 0
- slots_b: int32 [512, 8], P(('dp', 'ep')), parts along dimension 0
- gates_b: bfloat16 [512, 8], P(('dp', 'ep')), parts along dimension 0
- attn_gain: bfloat16 [1536], replicated
- w_query: bfloat16 [1536, 24, 64], replicated
- w_key: bfloat16 [1536, 24, 64], replicated
- w_value: bfloat16 [1536, 24, 64], replicated
- w_out: bfloat16 [24, 64, 1536], replicated
- moe_gain: bfloat16 [1536], replicated
- w_gate: bfloat16 [40, 1536, 512], P('ep')
- w_up: bfloat16 [40, 1536, 512], P('ep')
- w_down: bfloat16 [40, 512, 1536], P('ep')
Outputs:
- output 1: bfloat16 [512, 1536], P(('dp', 'ep')), parts along dimension 0
- output 2: bfloat16 [512, 1536], P(('dp', 'ep')), parts along dimension 0
There are 4 independent parts. The reference program is written for one: setup_inputs(seed, part) draws one part's arguments, and reference() takes and returns one part's arrays. A program takes and returns all parts, laid end to end along the dimension named above; an argument that names none is the same for every part.
All inputs are finite; a program needn't handle non-finite values.
Results may differ from the reference program's by a relative error of at most 0.0137052.
Values are sent between devices in bfloat16 or wider.
A program may use at most 1 GiB of HBM per device.

```python
import jax
import jax.numpy as jnp
from jax import lax

MODEL_DIM = 1536
FFN_DIM = 512
EXPERTS = 40
TOP_K = 8
HEADS = 24
TOKENS = 32
GROUP = 4
SLOTS = 8

HEAD_DIM = MODEL_DIM // HEADS
ROWS = GROUP * TOKENS
NORM_EPS = 1e-6
MASK_VALUE = -1e30


def draw_routing(route_key):
    key_start, key_hot, key_pick = jax.random.split(route_key, 3)
    spacing = EXPERTS // TOP_K
    hot_span = max(1, EXPERTS // (4 * TOP_K))
    start_any = jax.random.randint(key_start, (ROWS,), 0, EXPERTS)
    start_hot = jax.random.randint(key_hot, (ROWS,), 0, hot_span)
    use_hot = jax.random.randint(key_pick, (ROWS,), 0, 2) == 1
    position = jnp.arange(ROWS) % TOKENS
    first_expert = jnp.where(use_hot, start_hot, start_any)
    first_expert = jnp.where(position <= SLOTS, 0, first_expert)
    choice = (first_expert[:, None] + spacing * jnp.arange(TOP_K)[None, :]) % EXPERTS
    choice = choice.astype(jnp.int32)

    def device_slots(dev_choice):
        flat_ids = dev_choice.reshape(-1)
        onehot = (flat_ids[:, None] == jnp.arange(EXPERTS)[None, :]).astype(jnp.int32)
        rank_pos = jnp.sum(jnp.cumsum(onehot, axis=0) * onehot, axis=1) - 1
        return jnp.where(rank_pos < SLOTS, rank_pos, -1).reshape(TOKENS, TOP_K)

    slot_ids = lax.map(device_slots, choice.reshape(GROUP, TOKENS, TOP_K))
    return choice, slot_ids.reshape(ROWS, TOP_K).astype(jnp.int32)


def setup_inputs(seed: int = 0, part: int = 0) -> dict:
    base_key = jax.random.key(seed)
    part_key = jax.random.fold_in(base_key, part)
    part_keys = jax.random.split(part_key, 6)
    shared_keys = jax.random.split(base_key, 9)
    scale_in = MODEL_DIM ** -0.5
    scale_ffn = FFN_DIM ** -0.5
    experts_a, slots_a = draw_routing(part_keys[1])
    experts_b, slots_b = draw_routing(part_keys[4])
    return {
        "tokens_a": jax.random.normal(part_keys[0], (ROWS, MODEL_DIM), jnp.float32).astype(jnp.bfloat16),
        "experts_a": experts_a,
        "slots_a": slots_a,
        "gates_a": jax.random.uniform(part_keys[2], (ROWS, TOP_K), jnp.float32, 0.5, 1.5).astype(jnp.bfloat16),
        "tokens_b": jax.random.normal(part_keys[3], (ROWS, MODEL_DIM), jnp.float32).astype(jnp.bfloat16),
        "experts_b": experts_b,
        "slots_b": slots_b,
        "gates_b": jax.random.uniform(part_keys[5], (ROWS, TOP_K), jnp.float32, 0.5, 1.5).astype(jnp.bfloat16),
        "attn_gain": (1.0 + 0.3 * jax.random.normal(shared_keys[0], (MODEL_DIM,), jnp.float32)).astype(jnp.bfloat16),
        "w_query": (1.5 * scale_in * jax.random.normal(shared_keys[1], (MODEL_DIM, HEADS, HEAD_DIM), jnp.float32)).astype(jnp.bfloat16),
        "w_key": (1.5 * scale_in * jax.random.normal(shared_keys[2], (MODEL_DIM, HEADS, HEAD_DIM), jnp.float32)).astype(jnp.bfloat16),
        "w_value": (scale_in * jax.random.normal(shared_keys[3], (MODEL_DIM, HEADS, HEAD_DIM), jnp.float32)).astype(jnp.bfloat16),
        "w_out": (scale_in * jax.random.normal(shared_keys[4], (HEADS, HEAD_DIM, MODEL_DIM), jnp.float32)).astype(jnp.bfloat16),
        "moe_gain": (1.0 + 0.3 * jax.random.normal(shared_keys[5], (MODEL_DIM,), jnp.float32)).astype(jnp.bfloat16),
        "w_gate": (scale_in * jax.random.normal(shared_keys[6], (EXPERTS, MODEL_DIM, FFN_DIM), jnp.float32)).astype(jnp.bfloat16),
        "w_up": (scale_in * jax.random.normal(shared_keys[7], (EXPERTS, MODEL_DIM, FFN_DIM), jnp.float32)).astype(jnp.bfloat16),
        "w_down": (scale_ffn * jax.random.normal(shared_keys[8], (EXPERTS, FFN_DIM, MODEL_DIM), jnp.float32)).astype(jnp.bfloat16),
    }


def rms_norm(rows, gain_vec):
    rows_f = rows.astype(jnp.float32)
    inv_rms = lax.rsqrt(jnp.mean(rows_f * rows_f, axis=-1, keepdims=True) + NORM_EPS)
    return (rows_f * inv_rms * gain_vec.astype(jnp.float32)).astype(jnp.bfloat16)


def attention_block(sequence, attn_gain, w_query, w_key, w_value, w_out):
    normed = rms_norm(sequence, attn_gain).astype(jnp.float32)
    query = jnp.einsum("td,dhe->the", normed, w_query.astype(jnp.float32)).astype(jnp.bfloat16)
    keys = jnp.einsum("td,dhe->the", normed, w_key.astype(jnp.float32)).astype(jnp.bfloat16)
    values = jnp.einsum("td,dhe->the", normed, w_value.astype(jnp.float32)).astype(jnp.bfloat16)
    scores = jnp.einsum("qhe,khe->hqk", query.astype(jnp.float32), keys.astype(jnp.float32)) * (HEAD_DIM ** -0.5)
    causal = jnp.arange(TOKENS)[:, None] >= jnp.arange(TOKENS)[None, :]
    scores = jnp.where(causal[None, :, :], scores, MASK_VALUE)
    attn_prob = jax.nn.softmax(scores, axis=-1).astype(jnp.bfloat16)
    context = jnp.einsum("hqk,khe->qhe", attn_prob.astype(jnp.float32), values.astype(jnp.float32)).astype(jnp.bfloat16)
    attn_out = jnp.einsum("qhe,hed->qd", context.astype(jnp.float32), w_out.astype(jnp.float32))
    return (sequence.astype(jnp.float32) + attn_out).astype(jnp.bfloat16)


def moe_layer(tokens, experts, slots, gates, attn_gain, w_query, w_key, w_value, w_out, moe_gain, w_gate, w_up, w_down):
    residual = lax.map(lambda sequence: attention_block(sequence, attn_gain, w_query, w_key, w_value, w_out), tokens.reshape(GROUP, TOKENS, MODEL_DIM))
    normed = rms_norm(residual, moe_gain).reshape(ROWS, MODEL_DIM)
    row_ids = jnp.arange(ROWS, dtype=jnp.int32)
    owner = row_ids // TOKENS
    buffer_rows = EXPERTS * GROUP * SLOTS
    dest_row = jnp.where(slots >= 0, experts * (GROUP * SLOTS) + owner[:, None] * SLOTS + slots, buffer_rows)
    token_of = jnp.broadcast_to(row_ids[:, None], (ROWS, TOP_K)).reshape(-1)
    source = jnp.full((buffer_rows,), ROWS, jnp.int32).at[dest_row.reshape(-1)].set(token_of, mode="drop")

    def expert_ffn(operands):
        expert_source, gate_w, up_w, down_w = operands
        rows_in = jnp.take(normed, expert_source, axis=0, mode="fill", fill_value=0)
        gate_act = jnp.dot(rows_in, gate_w, preferred_element_type=jnp.float32)
        up_act = jnp.dot(rows_in, up_w, preferred_element_type=jnp.float32)
        hidden = (jax.nn.silu(gate_act) * up_act).astype(jnp.bfloat16)
        return jnp.dot(hidden, down_w, preferred_element_type=jnp.float32).astype(jnp.bfloat16)

    expert_out = lax.map(expert_ffn, (source.reshape(EXPERTS, GROUP * SLOTS), w_gate, w_up, w_down)).reshape(buffer_rows, MODEL_DIM)

    def combine(operands):
        dev_resid, dev_dest, dev_gates = operands
        picked = jnp.take(expert_out, dev_dest, axis=0, mode="fill", fill_value=0).reshape(TOKENS, TOP_K, MODEL_DIM)
        mixed_sum = jnp.einsum("tk,tkd->td", dev_gates.astype(jnp.float32), picked.astype(jnp.float32))
        return (dev_resid.astype(jnp.float32) + mixed_sum).astype(jnp.bfloat16)

    mixed_rows = lax.map(combine, (residual, dest_row.reshape(GROUP, TOKENS * TOP_K), gates.reshape(GROUP, TOKENS, TOP_K)))
    return mixed_rows.reshape(ROWS, MODEL_DIM)


def reference(tokens_a, experts_a, slots_a, gates_a, tokens_b, experts_b, slots_b, gates_b, attn_gain, w_query, w_key, w_value, w_out, moe_gain, w_gate, w_up, w_down):
    out_a = moe_layer(tokens_a, experts_a, slots_a, gates_a, attn_gain, w_query, w_key, w_value, w_out, moe_gain, w_gate, w_up, w_down)
    out_b = moe_layer(tokens_b, experts_b, slots_b, gates_b, attn_gain, w_query, w_key, w_value, w_out, moe_gain, w_gate, w_up, w_down)
    return (out_a, out_b)
```

```python
import functools

import jax
import jax.numpy as jnp
from jax import lax
from jax.experimental import pallas as pl
from jax.experimental.pallas import tpu as pltpu
from jax.sharding import PartitionSpec as P

NORM_EPS = 1e-6
MASK_VALUE = -1e30
MESH = pl.DeviceIdType.MESH

SEQ = 32
ROWS = 2 * SEQ
TOP_K = 8
DIM = 1536
HEAD = 64
FFN = 512
SLOTS = 8
LOCAL = 10
EXPERTS = 40
GROUP = 4
TOKENS = GROUP * ROWS
EROWS = GROUP * 2 * SLOTS
XROWS = LOCAL * EROWS
NB = 256
NBLK = DIM // NB
QCH = 512
NQ = 3 * DIM // QCH
NO = DIM // QCH

NT = (((1,), (1,)), ((), ()))
NN = (((1,), (0,)), ((), ()))


def dot(lhs, rhs, dims=NN):
    return lax.dot_general(lhs, rhs, dims, preferred_element_type=jnp.float32)


def rms_norm(rows_f, gain):
    inv_rms = lax.rsqrt(jnp.mean(rows_f * rows_f, axis=-1, keepdims=True) + NORM_EPS)
    return (rows_f * inv_rms * gain).astype(jnp.bfloat16)


def layer_kernel(
    tok_a, exp_a, slot_a, gate_a, tok_b, exp_b, slot_b, gate_b, again_h, mgain_h, wq, wk, wv, wo, wg, wu, wd,
    out_a, out_b,
    x_v, exp_v, slot_v, gate_v, again, mgain, buf1, wo_v, wg_v, wu_v, qkv, ctx, resid, u_all, codes, gts, disp, comb, xg, hid, o_v,
    p_send, p_recv, s_send, r_recv, keep, out_v,
    in_sem, q_sem, o_sem, g_sem, d_sem, out_sem, c_send, c_recv, u_send, u_recv, ps_sem, pr_sem, ss_sem, rr_sem,
):
    me = lax.axis_index("ep")
    dp = lax.axis_index("dp")
    x_pos = me // 2
    core = lax.rem(me, 2)
    sib = (dp, x_pos * 2 + (1 - core))
    cross = (dp, (1 - x_pos) * 2 + core)

    ins = []
    for i, (src, dst) in enumerate([
        (tok_a, x_v.at[pl.ds(0, SEQ)]), (tok_b, x_v.at[pl.ds(SEQ, SEQ)]), (again_h, again),
        (exp_a, exp_v.at[0]), (exp_b, exp_v.at[1]), (slot_a, slot_v.at[0]), (slot_b, slot_v.at[1]),
        (gate_a, gate_v.at[0]), (gate_b, gate_v.at[1]), (mgain_h, mgain),
    ]):
        cp = pltpu.make_async_copy(src, dst, in_sem.at[i])
        cp.start()
        ins.append(cp)

    q_cp = []
    for i in range(NQ):
        w, r = [(wq, 0), (wk, 1), (wv, 2)][i // (DIM // QCH)][0], i % (DIM // QCH)
        cp = pltpu.make_async_copy(w.at[pl.ds(r * QCH, QCH)], buf1.at[pl.ds(i * QCH, QCH)], q_sem.at[i])
        cp.start(priority=1)
        q_cp.append(cp)
    o_cp = []
    for i in range(NO):
        cp = pltpu.make_async_copy(wo.at[pl.ds(i * QCH, QCH)], wo_v.at[pl.ds(i * QCH, QCH)], o_sem.at[i])
        cp.start(priority=1)
        o_cp.append(cp)
    for e in range(LOCAL):
        pltpu.make_async_copy(wg.at[e], wg_v.at[e], g_sem.at[0, e]).start(priority=1)
        pltpu.make_async_copy(wu.at[e], wu_v.at[e], g_sem.at[1, e]).start(priority=1)

    barrier = pltpu.get_barrier_semaphore()
    for peer in (sib, cross):
        pl.semaphore_signal(barrier, inc=1, device_id=peer, device_id_type=MESH)

    for cp in ins:
        cp.wait()

    for b in range(2):
        s = slot_v[b]
        codes[0, b] = jnp.where(s >= 0, exp_v[b] * SLOTS + s, -1)
        gts[0, b] = gate_v[b].astype(jnp.float32)

    pl.semaphore_wait(barrier, 2)

    def remote(src, dst, ssem, rsem, dev):
        return pltpu.make_async_remote_copy(src_ref=src, dst_ref=dst, send_sem=ssem, recv_sem=rsem, device_id=dev, device_id_type=MESH)

    def exchange(buf, ssem, rsem):
        to_cross = remote(buf.at[0], buf.at[1], ssem.at[0], rsem.at[0], cross)
        to_sib = remote(buf.at[0], buf.at[2], ssem.at[1], rsem.at[1], sib)
        relay = remote(buf.at[1], buf.at[3], ssem.at[2], rsem.at[2], sib)
        return to_cross, to_sib, relay

    c_copies = exchange(codes, c_send.at[0], c_recv.at[0])
    g_copies = exchange(gts, c_send.at[1], c_recv.at[1])
    for cp in (*c_copies[:2], *g_copies[:2]):
        cp.start()

    x_f = x_v[...].astype(jnp.float32)
    normed = rms_norm(x_f, again[...].astype(jnp.float32).reshape(1, DIM))
    for i in range(NQ):
        q_cp[i].wait()
        qkv[i] = dot(normed, buf1[pl.ds(i * QCH, QCH), :], NT).astype(jnp.bfloat16)

    d_cp = []
    for n in range(NBLK):
        cp = pltpu.make_async_copy(wd.at[:, pl.ds(n * NB, NB)], buf1.at[:, pl.ds(n * NB, NB)], d_sem.at[n])
        cp.start(priority=1)
        d_cp.append(cp)

    c_copies[0].wait_recv()
    c_copies[2].start()
    g_copies[0].wait_recv()
    g_copies[2].start()

    q_row = lax.rem(lax.broadcasted_iota(jnp.int32, (4 * ROWS, ROWS), 0), ROWS)
    k_col = lax.broadcasted_iota(jnp.int32, (4 * ROWS, ROWS), 1)
    seen = (k_col <= q_row) & (k_col // SEQ == q_row // SEQ)
    lane_head = lax.broadcasted_iota(jnp.int32, (ROWS, 4 * HEAD), 1) // HEAD
    per = QCH // 256
    for g in range(DIM // 256):
        part = pl.ds((g % per) * 256, 256)
        q4 = qkv[g // per, :, part]
        k4 = qkv[NQ // 3 + g // per, :, part]
        v4 = qkv[2 * NQ // 3 + g // per, :, part]
        zero = jnp.zeros_like(q4)
        q_blocks = jnp.concatenate([jnp.where(lane_head == h, q4, zero) for h in range(4)], axis=0)
        s = dot(q_blocks, k4, NT) * (HEAD ** -0.5)
        s = jnp.where(seen, s, MASK_VALUE)
        ex = jnp.exp(s - jnp.max(s, axis=-1, keepdims=True))
        prob = (ex / jnp.sum(ex, axis=-1, keepdims=True)).astype(jnp.bfloat16)
        mixed = dot(prob, v4)
        c4 = mixed[0:ROWS]
        for h in range(1, 4):
            c4 = jnp.where(lane_head == h, mixed[h * ROWS:(h + 1) * ROWS], c4)
        ctx[:, pl.ds(g * 256, 256)] = c4.astype(jnp.bfloat16)

    for cp in o_cp:
        cp.wait()
    h = (x_f + dot(ctx[...], wo_v[...])).astype(jnp.bfloat16)
    resid[...] = h
    u_all[0] = rms_norm(h.astype(jnp.float32), mgain[...].astype(jnp.float32).reshape(1, DIM))

    u_copies = exchange(u_all, u_send, u_recv)
    u_copies[0].start()
    u_copies[1].start()

    for cp in (c_copies[1], c_copies[2], g_copies[1], g_copies[2]):
        cp.wait_recv()
    code = jnp.concatenate([codes[r, b] for r in range(GROUP) for b in range(2)], axis=1)
    gate = jnp.concatenate([gts[r, b] for r in range(GROUP) for b in range(2)], axis=1)
    block = lax.broadcasted_iota(jnp.int32, (TOP_K, TOKENS), 1) // SEQ
    code = jnp.where(code >= 0, code + block * (EXPERTS * SLOTS), -1)
    row = lax.broadcasted_iota(jnp.int32, (EROWS, TOKENS), 0)
    row_code = (row // SLOTS) * (EXPERTS * SLOTS) + lax.rem(row, SLOTS) + me * (LOCAL * SLOTS)

    def build(e, carry):
        want = row_code + e * SLOTS
        val = jnp.zeros((EROWS, TOKENS), jnp.float32)
        hit = jnp.zeros((EROWS, TOKENS), jnp.float32)
        for j in range(TOP_K):
            same = jnp.broadcast_to(code[j:j + 1, :], (EROWS, TOKENS)) == want
            val = jnp.where(same, jnp.broadcast_to(gate[j:j + 1, :], (EROWS, TOKENS)), val)
            hit = jnp.where(same, 1.0, hit)
        rows = pl.ds(pl.multiple_of(e * EROWS, EROWS), EROWS)
        disp[rows, :] = hit.astype(jnp.bfloat16)
        comb[rows, :] = val.astype(jnp.bfloat16)
        return carry

    lax.fori_loop(0, LOCAL, build, 0)
    comb_t = comb[...].T

    u_copies[0].wait_recv()
    u_copies[2].start()
    u_copies[1].wait_recv()
    u_copies[2].wait_recv()

    everyone = u_all[...].reshape(TOKENS, DIM)
    for n in range(DIM // 512):
        xg[:, pl.ds(n * 512, 512)] = dot(disp[...], everyone[:, n * 512:(n + 1) * 512]).astype(jnp.bfloat16)

    def expert(e, carry):
        pltpu.make_async_copy(wg.at[e], wg_v.at[e], g_sem.at[0, e]).wait()
        pltpu.make_async_copy(wu.at[e], wu_v.at[e], g_sem.at[1, e]).wait()
        rows = pl.ds(pl.multiple_of(e * EROWS, EROWS), EROWS)
        xe = xg[rows, :]
        gate_act = dot(xe, wg_v[e])
        up_act = dot(xe, wu_v[e])
        hid[rows, :] = (jax.nn.silu(gate_act) * up_act).astype(jnp.bfloat16)
        return carry

    lax.fori_loop(0, LOCAL, expert, 0)

    sends = []
    second = []

    def forward(n):
        first = sends[n]
        first.wait_recv()
        s_send[n] = s_send[n] + p_recv[n, pl.ds(ROWS, ROWS), :]
        cp = remote(s_send.at[n], r_recv.at[n], ss_sem.at[n], rr_sem.at[n], cross)
        cp.start()
        second.append(cp)

    for n in range(NBLK):
        cols = pl.ds(n * NB, NB)
        d_cp[n].wait()
        for e in range(LOCAL):
            o_v[pl.ds(e * EROWS, EROWS), :] = dot(hid[pl.ds(e * EROWS, EROWS), :], buf1[pl.ds(e * FFN, FFN), cols]).astype(jnp.bfloat16)
        part = dot(comb_t, o_v[...])
        keep[:, cols] = resid[:, cols].astype(jnp.float32) + part[0:ROWS]
        s_send[n] = part[ROWS:2 * ROWS]
        p_send[n] = part[2 * ROWS:]
        cp = remote(p_send.at[n], p_recv.at[n], ps_sem.at[n], pr_sem.at[n], sib)
        cp.start()
        sends.append(cp)
        if n >= 1:
            forward(n - 1)
    forward(NBLK - 1)

    for n in range(NBLK):
        cols = pl.ds(n * NB, NB)
        second[n].wait_recv()
        out_v[:, cols] = (keep[:, cols] + p_recv[n, pl.ds(0, ROWS), :] + r_recv[n]).astype(jnp.bfloat16)

    outs = [
        pltpu.make_async_copy(out_v.at[pl.ds(0, SEQ)], out_a, out_sem.at[0]),
        pltpu.make_async_copy(out_v.at[pl.ds(SEQ, SEQ)], out_b, out_sem.at[1]),
    ]
    for cp in outs:
        cp.start()
    for cp in (*c_copies, *g_copies, *u_copies, *sends, *second):
        cp.wait_send()
    for cp in outs:
        cp.wait()


def device_fn(tokens_a, experts_a, slots_a, gates_a, tokens_b, experts_b, slots_b, gates_b, attn_gain, w_query, w_key, w_value, w_out, moe_gain, w_gate, w_up, w_down):
    def by_row(w):
        return jnp.transpose(w, (1, 2, 0)).reshape(DIM, DIM)

    operands = (
        tokens_a, experts_a.T, slots_a.T, gates_a.T, tokens_b, experts_b.T, slots_b.T, gates_b.T, attn_gain, moe_gain,
        by_row(w_query), by_row(w_key), by_row(w_value), w_out.reshape(DIM, DIM), w_gate, w_up, w_down.reshape(LOCAL * FFN, DIM),
    )
    bf16, f32, i32 = jnp.bfloat16, jnp.float32, jnp.int32
    dma = pltpu.SemaphoreType.DMA
    scratch = [
        pltpu.VMEM((ROWS, DIM), bf16), pltpu.VMEM((2, TOP_K, SEQ), i32), pltpu.VMEM((2, TOP_K, SEQ), i32), pltpu.VMEM((2, TOP_K, SEQ), bf16),
        pltpu.VMEM((DIM,), bf16), pltpu.VMEM((DIM,), bf16),
        pltpu.VMEM((LOCAL * FFN, DIM), bf16), pltpu.VMEM((DIM, DIM), bf16), pltpu.VMEM((LOCAL, DIM, FFN), bf16), pltpu.VMEM((LOCAL, DIM, FFN), bf16),
        pltpu.VMEM((NQ, ROWS, QCH), bf16), pltpu.VMEM((ROWS, DIM), bf16), pltpu.VMEM((ROWS, DIM), bf16), pltpu.VMEM((GROUP, ROWS, DIM), bf16),
        pltpu.VMEM((GROUP, 2, TOP_K, SEQ), i32), pltpu.VMEM((GROUP, 2, TOP_K, SEQ), f32),
        pltpu.VMEM((XROWS, TOKENS), bf16), pltpu.VMEM((XROWS, TOKENS), bf16), pltpu.VMEM((XROWS, DIM), bf16), pltpu.VMEM((XROWS, FFN), bf16),
        pltpu.VMEM((XROWS, NB), bf16),
        pltpu.VMEM((NBLK, 2 * ROWS, NB), f32), pltpu.VMEM((NBLK, 2 * ROWS, NB), f32), pltpu.VMEM((NBLK, ROWS, NB), f32), pltpu.VMEM((NBLK, ROWS, NB), f32),
        pltpu.VMEM((ROWS, DIM), f32), pltpu.VMEM((ROWS, DIM), bf16),
        dma((10,)), dma((NQ,)), dma((NO,)), dma((2, LOCAL)), dma((NBLK,)), dma((2,)),
        dma((2, 3)), dma((2, 3)), dma((3,)), dma((3,)), dma((NBLK,)), dma((NBLK,)), dma((NBLK,)), dma((NBLK,)),
    ]
    shape = jax.ShapeDtypeStruct((SEQ, DIM), bf16)
    return pl.pallas_call(
        layer_kernel,
        out_shape=(shape, shape),
        in_specs=[pl.BlockSpec(memory_space=pl.ANY)] * len(operands),
        out_specs=[pl.BlockSpec(memory_space=pl.ANY)] * 2,
        scratch_shapes=scratch,
        compiler_params=pltpu.CompilerParams(collective_id=0, has_side_effects=True, vmem_limit_bytes=66_000_000),
        name="moe_layer",
    )(*operands)


def solution(mesh):
    row_spec = P(("dp", "ep"), None)
    full_spec = P(None, None, None)
    gain_spec = P(None)
    expert_spec = P("ep", None, None)
    in_specs = (row_spec, row_spec, row_spec, row_spec, row_spec, row_spec, row_spec, row_spec, gain_spec, full_spec, full_spec, full_spec, full_spec, gain_spec, expert_spec, expert_spec, expert_spec)
    return jax.shard_map(device_fn, mesh=mesh, in_specs=in_specs, out_specs=(row_spec, row_spec), check_vma=False)
```

```python
import functools

import jax
import jax.numpy as jnp
from jax import lax
from jax.experimental import pallas as pl
from jax.experimental.pallas import tpu as pltpu
from jax.sharding import PartitionSpec as P

NORM_EPS = 1e-6
MASK_VALUE = -1e30
MESH = pl.DeviceIdType.MESH
VMEM_LIMIT = 65_000_000

SEQ = 32
ROWS = 2 * SEQ
TOP_K = 8
DIM = 1536
HEAD = 64
FFN = 512
SLOTS = 8
LOCAL = 10
EXPERTS = 40
GROUP = 4
TOKENS = GROUP * ROWS
EROWS = GROUP * 2 * SLOTS
RROWS = LOCAL * 2 * SLOTS
NB = 256
NBLK = DIM // NB
QCH = 768
PER = DIM // QCH
NQ = 3 * PER

NT = (((1,), (1,)), ((), ()))
NN = (((1,), (0,)), ((), ()))


def dot(lhs, rhs, dims=NN):
    return lax.dot_general(lhs, rhs, dims, preferred_element_type=jnp.float32)


def rms_norm(rows_f, gain):
    inv_rms = lax.rsqrt(jnp.mean(rows_f * rows_f, axis=-1, keepdims=True) + NORM_EPS)
    return (rows_f * inv_rms * gain).astype(jnp.bfloat16)


def layer_kernel(
    tok_a, exp_a, slot_a, gate_a, tok_b, exp_b, slot_b, gate_b, again_h, mgain_h, wq, wk, wv, wo, wg, wu, wd,
    out_h,
    x_v, exp_v, slot_v, gate_v, again, mgain, buf1, wo_v, wg_v, wu_v, qkv, ctx, u_all, codes, gts, disp, comb_t, xg, hid, o_v,
    p_send, p_recv, s_send, r_recv, keep, out_v,
    in_sem, q_sem, o_sem, g_sem, d_sem, out_sem, c_send, c_recv, u_send, u_recv, ps_sem, pr_sem, ss_sem, rr_sem,
):
    me = lax.axis_index("ep")
    dp = lax.axis_index("dp")
    x_pos = me // 2
    core = lax.rem(me, 2)
    sib = (dp, x_pos * 2 + (1 - core))
    cross = (dp, (1 - x_pos) * 2 + core)

    ins = []
    for i, (src, dst) in enumerate([
        (tok_a, x_v.at[pl.ds(0, SEQ)]), (tok_b, x_v.at[pl.ds(SEQ, SEQ)]), (again_h, again),
        (exp_a, exp_v.at[0]), (exp_b, exp_v.at[1]), (slot_a, slot_v.at[0]), (slot_b, slot_v.at[1]),
        (gate_a, gate_v.at[0]), (gate_b, gate_v.at[1]), (mgain_h, mgain),
    ]):
        cp = pltpu.make_async_copy(src, dst, in_sem.at[i])
        cp.start()
        ins.append(cp)

    q_cp = []
    for i in range(NQ):
        w, r = (wq, wk, wv)[i // PER], i % PER
        cp = pltpu.make_async_copy(w.at[pl.ds(r * QCH, QCH)], buf1.at[pl.ds(i * QCH, QCH)], q_sem.at[i])
        cp.start(priority=1)
        q_cp.append(cp)
    o_cp = pltpu.make_async_copy(wo, wo_v, o_sem.at[0])
    o_cp.start(priority=1)

    g_cp = [
        (pltpu.make_async_copy(wg.at[e], wg_v.at[e], g_sem.at[0, e]), pltpu.make_async_copy(wu.at[e], wu_v.at[e], g_sem.at[1, e]))
        for e in range(LOCAL)
    ]

    def fetch(first, last):
        for e in range(first, last):
            for cp in g_cp[e]:
                cp.start(priority=1)

    barrier = pltpu.get_barrier_semaphore()
    for peer in (sib, cross):
        pl.semaphore_signal(barrier, inc=1, device_id=peer, device_id_type=MESH)

    for cp in ins:
        cp.wait()

    for b in range(2):
        s = slot_v[b]
        codes[0, b] = jnp.where(s >= 0, exp_v[b] * SLOTS + s, -1)
        gts[0, b] = gate_v[b].astype(jnp.float32)

    def remote(src, dst, ssem, rsem, dev):
        return pltpu.make_async_remote_copy(src_ref=src, dst_ref=dst, send_sem=ssem, recv_sem=rsem, device_id=dev, device_id_type=MESH)

    def exchange(buf, ssem, rsem):
        to_cross = remote(buf.at[0], buf.at[1], ssem.at[0], rsem.at[0], cross)
        to_sib = remote(buf.at[0], buf.at[2], ssem.at[1], rsem.at[1], sib)
        relay = remote(buf.at[1], buf.at[3], ssem.at[2], rsem.at[2], sib)
        return to_cross, to_sib, relay

    x_f = x_v[...].astype(jnp.float32)
    normed = rms_norm(x_f, again[...].astype(jnp.float32).reshape(1, DIM))

    def project(first, last):
        rows = pl.ds(first * QCH, (last - first) * QCH)
        res = dot(normed, buf1[rows, :], NT).astype(jnp.bfloat16)
        for i in range(first, last):
            qkv[i] = res[:, (i - first) * QCH:(i - first + 1) * QCH]

    q_cp[0].wait()
    fetch(0, 1)
    project(0, 1)
    q_cp[1].wait()
    fetch(1, 2)
    project(1, 2)

    q_cp[2].wait()
    q_cp[3].wait()
    fetch(2, 4)
    project(2, 4)

    pl.semaphore_wait(barrier, 2)
    c_copies = exchange(codes, c_send.at[0], c_recv.at[0])
    g_copies = exchange(gts, c_send.at[1], c_recv.at[1])
    for cp in (*c_copies[:2], *g_copies[:2]):
        cp.start()

    q_cp[4].wait()
    q_cp[5].wait()
    fetch(4, LOCAL)
    q_row = lax.rem(lax.broadcasted_iota(jnp.int32, (4 * ROWS, ROWS), 0), ROWS)
    k_col = lax.broadcasted_iota(jnp.int32, (4 * ROWS, ROWS), 1)
    seen = (k_col <= q_row) & (k_col // SEQ == q_row // SEQ)
    lane_head = lax.broadcasted_iota(jnp.int32, (ROWS, 4 * HEAD), 1) // HEAD
    groups = QCH // 256
    probs = []
    for g in range(DIM // 256):
        part = pl.ds((g % groups) * 256, 256)
        q4 = qkv[g // groups, :, part]
        k4 = qkv[PER + g // groups, :, part]
        zero = jnp.zeros_like(q4)
        q_blocks = jnp.concatenate([jnp.where(lane_head == h, q4, zero) for h in range(4)], axis=0)
        s = dot(q_blocks, k4, NT) * (HEAD ** -0.5)
        s = jnp.where(seen, s, MASK_VALUE)
        ex = jnp.exp(s - jnp.max(s, axis=-1, keepdims=True))
        probs.append((ex / jnp.sum(ex, axis=-1, keepdims=True)).astype(jnp.bfloat16))
    project(4, 6)
    for g in range(DIM // 256):
        v4 = qkv[2 * PER + g // groups, :, pl.ds((g % groups) * 256, 256)]
        mixed = dot(probs[g], v4)
        c4 = mixed[0:ROWS]
        for h in range(1, 4):
            c4 = jnp.where(lane_head == h, mixed[h * ROWS:(h + 1) * ROWS], c4)
        ctx[:, pl.ds(g * 256, 256)] = c4.astype(jnp.bfloat16)

    o_cp.wait()
    h = (x_f + dot(ctx[...], wo_v[...])).astype(jnp.bfloat16)
    keep[...] = h.astype(jnp.float32)
    u_all[0] = rms_norm(h.astype(jnp.float32), mgain[...].astype(jnp.float32).reshape(1, DIM))

    u_copies = exchange(u_all, u_send, u_recv)
    u_copies[0].start()
    u_copies[1].start()

    d_cp = []
    for n in range(NBLK):
        cp = pltpu.make_async_copy(wd.at[:, pl.ds(n * NB, NB)], buf1.at[:, pl.ds(n * NB, NB)], d_sem.at[n])
        cp.start(priority=1)
        d_cp.append(cp)

    c_copies[0].wait_recv()
    c_copies[2].start()
    g_copies[0].wait_recv()
    g_copies[2].start()
    for cp in (c_copies[1], g_copies[1], c_copies[2], g_copies[2]):
        cp.wait_recv()
    row = lax.broadcasted_iota(jnp.int32, (RROWS, ROWS), 0)
    want = (row // (2 * SLOTS) + me * LOCAL) * SLOTS + lax.rem(row, SLOTS) + lax.rem(row // SLOTS, 2) * (EXPERTS * SLOTS)
    for r in range(GROUP):
        code = jnp.concatenate([codes[r, 0], jnp.where(codes[r, 1] >= 0, codes[r, 1] + EXPERTS * SLOTS, -1)], axis=1)
        gate = jnp.concatenate([gts[r, 0], gts[r, 1]], axis=1)
        val = jnp.zeros((RROWS, ROWS), jnp.float32)
        hit = jnp.zeros((RROWS, ROWS), jnp.float32)
        for j in range(TOP_K):
            same = jnp.broadcast_to(code[j:j + 1, :], (RROWS, ROWS)) == want
            val = jnp.where(same, jnp.broadcast_to(gate[j:j + 1, :], (RROWS, ROWS)), val)
            hit = jnp.where(same, 1.0, hit)
        disp[r] = hit.astype(jnp.bfloat16)
        comb_t[r] = val.T.astype(jnp.bfloat16)

    def gather(r):
        xg[r] = dot(disp[r], u_all[r]).astype(jnp.bfloat16).reshape(LOCAL, 2 * SLOTS, DIM)

    gather(0)
    u_copies[1].wait_recv()
    gather(2)
    u_copies[0].wait_recv()
    u_copies[2].start()
    gather(1)
    u_copies[2].wait_recv()
    gather(3)

    def expert(e):
        xe = xg[:, e].reshape(EROWS, DIM)
        gate_act = dot(xe, wg_v[e])
        up_act = dot(xe, wu_v[e])
        hid[:, e] = (jax.nn.silu(gate_act) * up_act).astype(jnp.bfloat16).reshape(GROUP, 2 * SLOTS, FFN)

    for first, last in ((0, 7), (7, LOCAL)):
        for e in range(first, last):
            for cp in g_cp[e]:
                cp.wait()
        for e in range(first, last):
            expert(e)

    sends = []
    second = []

    def forward(n):
        sends[n].wait_recv()
        s_send[n] = s_send[n] + p_recv[n, 1]
        cp = remote(s_send.at[n], r_recv.at[n], ss_sem.at[n], rr_sem.at[n], cross)
        cp.start()
        second.append(cp)

    def down(n):
        cols = pl.ds(n * NB, NB)
        for e in range(LOCAL):
            res = dot(hid[:, e].reshape(EROWS, FFN), buf1[pl.ds(e * FFN, FFN), cols])
            o_v[n % 2, :, e] = res.astype(jnp.bfloat16).reshape(GROUP, 2 * SLOTS, NB)

    def combine(n, r):
        return dot(comb_t[r], o_v[n % 2, r].reshape(RROWS, NB))

    d_cp[0].wait()
    down(0)
    for n in range(NBLK):
        if n + 1 < NBLK:
            d_cp[n + 1].wait()
        p_send[n, 1] = combine(n, 3)
        p_send[n, 0] = combine(n, 2)
        s_send[n] = combine(n, 1)
        cols = pl.ds(n * NB, NB)
        keep[:, cols] = keep[:, cols] + combine(n, 0)
        if n + 1 < NBLK:
            down(n + 1)
        cp = remote(p_send.at[n], p_recv.at[n], ps_sem.at[n], pr_sem.at[n], sib)
        cp.start()
        sends.append(cp)
        if n >= 1:
            forward(n - 1)
    forward(NBLK - 1)

    for n in range(NBLK):
        cols = pl.ds(n * NB, NB)
        second[n].wait_recv()
        out_v[:, cols] = (keep[:, cols] + p_recv[n, 0] + r_recv[n]).astype(jnp.bfloat16)

    out_cp = pltpu.make_async_copy(out_v, out_h, out_sem.at[0])
    out_cp.start()
    for cp in (*c_copies, *g_copies, *u_copies, *sends, *second):
        cp.wait_send()
    out_cp.wait()


def device_fn(tokens_a, experts_a, slots_a, gates_a, tokens_b, experts_b, slots_b, gates_b, attn_gain, w_query, w_key, w_value, w_out, moe_gain, w_gate, w_up, w_down):
    def by_row(w):
        return jnp.transpose(w, (1, 2, 0)).reshape(DIM, DIM)

    operands = (
        tokens_a, experts_a.T, slots_a.T, gates_a.T, tokens_b, experts_b.T, slots_b.T, gates_b.T, attn_gain, moe_gain,
        by_row(w_query), by_row(w_key), by_row(w_value), w_out.reshape(DIM, DIM), w_gate, w_up, w_down.reshape(LOCAL * FFN, DIM),
    )
    bf16, f32, i32 = jnp.bfloat16, jnp.float32, jnp.int32
    dma = pltpu.SemaphoreType.DMA
    scratch = [
        pltpu.VMEM((ROWS, DIM), bf16), pltpu.VMEM((2, TOP_K, SEQ), i32), pltpu.VMEM((2, TOP_K, SEQ), i32), pltpu.VMEM((2, TOP_K, SEQ), bf16),
        pltpu.VMEM((DIM,), bf16), pltpu.VMEM((DIM,), bf16),
        pltpu.VMEM((LOCAL * FFN, DIM), bf16), pltpu.VMEM((DIM, DIM), bf16), pltpu.VMEM((LOCAL, DIM, FFN), bf16), pltpu.VMEM((LOCAL, DIM, FFN), bf16),
        pltpu.VMEM((NQ, ROWS, QCH), bf16), pltpu.VMEM((ROWS, DIM), bf16), pltpu.VMEM((GROUP, ROWS, DIM), bf16),
        pltpu.VMEM((GROUP, 2, TOP_K, SEQ), i32), pltpu.VMEM((GROUP, 2, TOP_K, SEQ), f32),
        pltpu.VMEM((GROUP, RROWS, ROWS), bf16), pltpu.VMEM((GROUP, ROWS, RROWS), bf16),
        pltpu.VMEM((GROUP, LOCAL, 2 * SLOTS, DIM), bf16), pltpu.VMEM((GROUP, LOCAL, 2 * SLOTS, FFN), bf16), pltpu.VMEM((2, GROUP, LOCAL, 2 * SLOTS, NB), bf16),
        pltpu.VMEM((NBLK, 2, ROWS, NB), f32), pltpu.VMEM((NBLK, 2, ROWS, NB), f32), pltpu.VMEM((NBLK, ROWS, NB), f32), pltpu.VMEM((NBLK, ROWS, NB), f32),
        pltpu.VMEM((ROWS, DIM), f32), pltpu.VMEM((ROWS, DIM), bf16),
        dma((10,)), dma((NQ,)), dma((1,)), dma((2, LOCAL)), dma((NBLK,)), dma((1,)),
        dma((2, 3)), dma((2, 3)), dma((3,)), dma((3,)), dma((NBLK,)), dma((NBLK,)), dma((NBLK,)), dma((NBLK,)),
    ]
    both = pl.pallas_call(
        layer_kernel,
        out_shape=jax.ShapeDtypeStruct((ROWS, DIM), bf16),
        in_specs=[pl.BlockSpec(memory_space=pl.ANY)] * len(operands),
        out_specs=pl.BlockSpec(memory_space=pl.ANY),
        scratch_shapes=scratch,
        compiler_params=pltpu.CompilerParams(collective_id=0, has_side_effects=True, vmem_limit_bytes=VMEM_LIMIT),
        name="moe_layer",
    )(*operands)
    return split(both)


def split_kernel(both, out_a, out_b, sem):
    copies = [pltpu.make_async_copy(both.at[pl.ds(i * SEQ, SEQ)], dst, sem.at[i]) for i, dst in enumerate((out_a, out_b))]
    for cp in copies:
        cp.start()
    for cp in copies:
        cp.wait()


def split(both):
    shape = jax.ShapeDtypeStruct((SEQ, DIM), jnp.bfloat16)
    return pl.pallas_call(
        split_kernel,
        out_shape=(shape, shape),
        in_specs=[pl.BlockSpec(memory_space=pltpu.VMEM)],
        out_specs=[pl.BlockSpec(memory_space=pl.ANY)] * 2,
        scratch_shapes=[pltpu.SemaphoreType.DMA((2,))],
        name="split",
    )(both)


def solution(mesh):
    row_spec = P(("dp", "ep"), None)
    full_spec = P(None, None, None)
    gain_spec = P(None)
    expert_spec = P("ep", None, None)
    in_specs = (row_spec, row_spec, row_spec, row_spec, row_spec, row_spec, row_spec, row_spec, gain_spec, full_spec, full_spec, full_spec, full_spec, gain_spec, expert_spec, expert_spec, expert_spec)
    return jax.shard_map(device_fn, mesh=mesh, in_specs=in_specs, out_specs=(row_spec, row_spec), check_vma=False)
```

```python
import functools

import jax
import jax.numpy as jnp
from jax import lax
from jax.experimental import pallas as pl
from jax.experimental.pallas import tpu as pltpu
from jax.sharding import PartitionSpec as P

NORM_EPS = 1e-6
MASK_VALUE = -1e30
MESH = pl.DeviceIdType.MESH
VMEM_LIMIT = 66_000_000

SEQ = 32
ROWS = 2 * SEQ
TOP_K = 8
DIM = 1536
HEAD = 64
FFN = 512
SLOTS = 8
LOCAL = 10
EXPERTS = 40
GROUP = 4
TOKENS = GROUP * ROWS
EROWS = GROUP * 2 * SLOTS
RROWS = LOCAL * 2 * SLOTS
KS = (256, 256, 512, 512)
KOFF = tuple(sum(KS[:k]) for k in range(len(KS)))
NB = 256
NBLK = DIM // NB
QCH = 768
PER = DIM // QCH
NQ = 3 * PER

NT = (((1,), (1,)), ((), ()))
NN = (((1,), (0,)), ((), ()))


def dot(lhs, rhs, dims=NN):
    return lax.dot_general(lhs, rhs, dims, preferred_element_type=jnp.float32)


def rms_norm(rows_f, gain):
    inv_rms = lax.rsqrt(jnp.mean(rows_f * rows_f, axis=-1, keepdims=True) + NORM_EPS)
    return (rows_f * inv_rms * gain).astype(jnp.bfloat16)


def layer_kernel(
    tok_a, exp_a, slot_a, gate_a, tok_b, exp_b, slot_b, gate_b, again_h, mgain_h, wq, wk, wv, wo, wg, wu, wd,
    out_h,
    x_v, exp_v, slot_v, gate_v, again, mgain, buf1, wo_v, wg_v, wu_v, qkv, ctx, u_all, codes, gts, disp, comb_t, xg, hid, o_v,
    p_send, p_recv, s_send, r_recv, keep, out_v, acc,
    in_sem, q_sem, o_sem, g_sem, d_sem, out_sem, c_send, c_recv, u_send, u_recv, ps_sem, pr_sem, ss_sem, rr_sem,
):
    me = lax.axis_index("ep")
    dp = lax.axis_index("dp")
    x_pos = me // 2
    core = lax.rem(me, 2)
    sib = (dp, x_pos * 2 + (1 - core))
    cross = (dp, (1 - x_pos) * 2 + core)

    ins = []
    for i, (src, dst) in enumerate([
        (tok_a, x_v.at[pl.ds(0, SEQ)]), (tok_b, x_v.at[pl.ds(SEQ, SEQ)]), (again_h, again),
        (exp_a, exp_v.at[0]), (exp_b, exp_v.at[1]), (slot_a, slot_v.at[0]), (slot_b, slot_v.at[1]),
        (gate_a, gate_v.at[0]), (gate_b, gate_v.at[1]), (mgain_h, mgain),
    ]):
        cp = pltpu.make_async_copy(src, dst, in_sem.at[i])
        cp.start()
        ins.append(cp)

    q_cp = []
    for i in range(NQ):
        w, r = (wq, wk, wv)[i // PER], i % PER
        cp = pltpu.make_async_copy(w.at[pl.ds(r * QCH, QCH)], buf1.at[pl.ds(i * QCH, QCH)], q_sem.at[i])
        cp.start(priority=1)
        q_cp.append(cp)
    o_cp = pltpu.make_async_copy(wo, wo_v, o_sem.at[0])
    o_cp.start(priority=1)

    g_cp = []
    for k, (off, size) in enumerate(zip(KOFF, KS)):
        ks = pl.ds(off, size)
        g_cp.append([pltpu.make_async_copy(w.at[:, ks, :], v.at[:, ks, :], g_sem.at[i, k]) for i, (w, v) in enumerate(((wg, wg_v), (wu, wu_v)))])

    def fetch(k):
        for cp in g_cp[k]:
            cp.start(priority=1)

    barrier = pltpu.get_barrier_semaphore()
    for peer in (sib, cross):
        pl.semaphore_signal(barrier, inc=1, device_id=peer, device_id_type=MESH)

    for cp in ins:
        cp.wait()

    for b in range(2):
        s = slot_v[b]
        codes[0, b] = jnp.where(s >= 0, exp_v[b] * SLOTS + s, -1)
        gts[0, b] = gate_v[b].astype(jnp.float32)

    def remote(src, dst, ssem, rsem, dev):
        return pltpu.make_async_remote_copy(src_ref=src, dst_ref=dst, send_sem=ssem, recv_sem=rsem, device_id=dev, device_id_type=MESH)

    def exchange(buf, ssem, rsem):
        to_cross = remote(buf.at[0], buf.at[1], ssem.at[0], rsem.at[0], cross)
        to_sib = remote(buf.at[0], buf.at[2], ssem.at[1], rsem.at[1], sib)
        relay = remote(buf.at[1], buf.at[3], ssem.at[2], rsem.at[2], sib)
        return to_cross, to_sib, relay

    x_f = x_v[...].astype(jnp.float32)
    normed = rms_norm(x_f, again[...].astype(jnp.float32).reshape(1, DIM))

    def project(first, last):
        rows = pl.ds(first * QCH, (last - first) * QCH)
        res = dot(normed, buf1[rows, :], NT).astype(jnp.bfloat16)
        for i in range(first, last):
            qkv[i] = res[:, (i - first) * QCH:(i - first + 1) * QCH]

    q_cp[0].wait()
    fetch(0)
    project(0, 1)
    q_cp[1].wait()
    fetch(1)
    project(1, 2)

    q_cp[2].wait()
    q_cp[3].wait()
    fetch(2)
    project(2, 4)

    pl.semaphore_wait(barrier, 2)
    c_copies = exchange(codes, c_send.at[0], c_recv.at[0])
    g_copies = exchange(gts, c_send.at[1], c_recv.at[1])
    for cp in (*c_copies[:2], *g_copies[:2]):
        cp.start()

    q_cp[4].wait()
    q_cp[5].wait()
    fetch(3)
    q_row = lax.rem(lax.broadcasted_iota(jnp.int32, (4 * ROWS, ROWS), 0), ROWS)
    k_col = lax.broadcasted_iota(jnp.int32, (4 * ROWS, ROWS), 1)
    seen = (k_col <= q_row) & (k_col // SEQ == q_row // SEQ)
    lane_head = lax.broadcasted_iota(jnp.int32, (ROWS, 4 * HEAD), 1) // HEAD
    groups = QCH // 256
    probs = []
    for g in range(DIM // 256):
        part = pl.ds((g % groups) * 256, 256)
        q4 = qkv[g // groups, :, part]
        k4 = qkv[PER + g // groups, :, part]
        zero = jnp.zeros_like(q4)
        q_blocks = jnp.concatenate([jnp.where(lane_head == h, q4, zero) for h in range(4)], axis=0)
        s = dot(q_blocks, k4, NT) * (HEAD ** -0.5)
        s = jnp.where(seen, s, MASK_VALUE)
        ex = jnp.exp(s - jnp.max(s, axis=-1, keepdims=True))
        probs.append((ex / jnp.sum(ex, axis=-1, keepdims=True)).astype(jnp.bfloat16))
    project(4, 6)
    for g in range(DIM // 256):
        v4 = qkv[2 * PER + g // groups, :, pl.ds((g % groups) * 256, 256)]
        mixed = dot(probs[g], v4)
        c4 = mixed[0:ROWS]
        for h in range(1, 4):
            c4 = jnp.where(lane_head == h, mixed[h * ROWS:(h + 1) * ROWS], c4)
        ctx[:, pl.ds(g * 256, 256)] = c4.astype(jnp.bfloat16)

    o_cp.wait()
    h = (x_f + dot(ctx[...], wo_v[...])).astype(jnp.bfloat16)
    keep[...] = h.astype(jnp.float32)
    u_all[0] = rms_norm(h.astype(jnp.float32), mgain[...].astype(jnp.float32).reshape(1, DIM))

    u_copies = []
    for k, (off, size) in enumerate(zip(KOFF, KS)):
        view = u_all.at[:, :, pl.ds(off, size)]
        u_copies.append(exchange(view, u_send.at[k], u_recv.at[k]))
        u_copies[k][0].start()
    for copies in u_copies:
        copies[1].start()

    d_cp = []
    for n in range(NBLK):
        cp = pltpu.make_async_copy(wd.at[:, pl.ds(n * NB, NB)], buf1.at[:, pl.ds(n * NB, NB)], d_sem.at[n])
        cp.start(priority=1)
        d_cp.append(cp)

    c_copies[0].wait_recv()
    c_copies[2].start()
    g_copies[0].wait_recv()
    g_copies[2].start()
    for cp in (c_copies[1], g_copies[1], c_copies[2], g_copies[2]):
        cp.wait_recv()
    row = lax.broadcasted_iota(jnp.int32, (RROWS, ROWS), 0)
    want = (row // (2 * SLOTS) + me * LOCAL) * SLOTS + lax.rem(row, SLOTS) + lax.rem(row // SLOTS, 2) * (EXPERTS * SLOTS)
    for r in range(GROUP):
        code = jnp.concatenate([codes[r, 0], jnp.where(codes[r, 1] >= 0, codes[r, 1] + EXPERTS * SLOTS, -1)], axis=1)
        gate = jnp.concatenate([gts[r, 0], gts[r, 1]], axis=1)
        val = jnp.zeros((RROWS, ROWS), jnp.float32)
        hit = jnp.zeros((RROWS, ROWS), jnp.float32)
        for j in range(TOP_K):
            same = jnp.broadcast_to(code[j:j + 1, :], (RROWS, ROWS)) == want
            val = jnp.where(same, jnp.broadcast_to(gate[j:j + 1, :], (RROWS, ROWS)), val)
            hit = jnp.where(same, 1.0, hit)
        disp[r] = hit.astype(jnp.bfloat16)
        comb_t[r] = val.T.astype(jnp.bfloat16)

    def gather(r, k):
        ks = pl.ds(KOFF[k], KS[k])
        xg[r, :, :, ks] = dot(disp[r], u_all[r, :, ks]).astype(jnp.bfloat16).reshape(LOCAL, 2 * SLOTS, KS[k])

    for k in range(len(KS)):
        gather(0, k)
    for k in range(len(KS)):
        u_copies[k][1].wait_recv()
    for k in range(len(KS)):
        gather(2, k)

    def relay(k):
        u_copies[k][0].wait_recv()
        u_copies[k][2].start()

    def experts(k, first, last):
        ks = pl.ds(KOFF[k], KS[k])
        for e in range(first, last):
            xe = xg[:, e, :, ks].reshape(EROWS, KS[k])
            gate_act = dot(xe, wg_v[e, ks, :])
            up_act = dot(xe, wu_v[e, ks, :])
            if k > 0:
                gate_act = acc[e, 0] + gate_act
                up_act = acc[e, 1] + up_act
            if k + 1 < len(KS):
                acc[e, 0] = gate_act
                acc[e, 1] = up_act
            else:
                hid[:, e] = (jax.nn.silu(gate_act) * up_act).astype(jnp.bfloat16).reshape(GROUP, 2 * SLOTS, FFN)

    relay(0)
    for k in range(len(KS)):
        gather(1, k)
        u_copies[k][2].wait_recv()
        for cp in g_cp[k]:
            cp.wait()
        gather(3, k)
        half = LOCAL // 2
        experts(k, 0, half)
        if k + 1 < len(KS):
            relay(k + 1)
        experts(k, half, LOCAL)

    sends = []
    second = []

    def forward(n):
        sends[n][0].wait_recv()
        s_send[n] = s_send[n] + p_recv[n, 1]
        cp = remote(s_send.at[n], r_recv.at[n], ss_sem.at[n], rr_sem.at[n], cross)
        cp.start()
        second.append(cp)

    def down(n):
        cols = pl.ds(n * NB, NB)
        for e in range(LOCAL):
            res = dot(hid[:, e].reshape(EROWS, FFN), buf1[pl.ds(e * FFN, FFN), cols])
            o_v[n % 2, :, e] = res.astype(jnp.bfloat16).reshape(GROUP, 2 * SLOTS, NB)

    def combine(n, r):
        return dot(comb_t[r], o_v[n % 2, r].reshape(RROWS, NB))

    d_cp[0].wait()
    down(0)
    for n in range(NBLK):
        if n + 1 < NBLK:
            d_cp[n + 1].wait()
        p_send[n, 1] = combine(n, 3)
        p_send[n, 0] = combine(n, 2)
        s_send[n] = combine(n, 1)
        cols = pl.ds(n * NB, NB)
        keep[:, cols] = keep[:, cols] + combine(n, 0)
        if n + 1 < NBLK:
            down(n + 1)
        sends.append([remote(p_send.at[n, i], p_recv.at[n, i], ps_sem.at[n, i], pr_sem.at[n, i], sib) for i in (1, 0)])
        for cp in sends[n]:
            cp.start()
        if n >= 1:
            forward(n - 1)
    forward(NBLK - 1)

    for n in range(NBLK):
        cols = pl.ds(n * NB, NB)
        sends[n][1].wait_recv()
        second[n].wait_recv()
        out_v[:, cols] = (keep[:, cols] + p_recv[n, 0] + r_recv[n]).astype(jnp.bfloat16)

    out_cp = pltpu.make_async_copy(out_v, out_h, out_sem.at[0])
    out_cp.start()
    for cp in (*c_copies, *g_copies, *(c for cs in u_copies for c in cs), *(c for cs in sends for c in cs), *second):
        cp.wait_send()
    out_cp.wait()


def device_fn(tokens_a, experts_a, slots_a, gates_a, tokens_b, experts_b, slots_b, gates_b, attn_gain, w_query, w_key, w_value, w_out, moe_gain, w_gate, w_up, w_down):
    def by_row(w):
        return jnp.transpose(w, (1, 2, 0)).reshape(DIM, DIM)

    operands = (
        tokens_a, experts_a.T, slots_a.T, gates_a.T, tokens_b, experts_b.T, slots_b.T, gates_b.T, attn_gain, moe_gain,
        by_row(w_query), by_row(w_key), by_row(w_value), w_out.reshape(DIM, DIM), w_gate, w_up, w_down.reshape(LOCAL * FFN, DIM),
    )
    bf16, f32, i32 = jnp.bfloat16, jnp.float32, jnp.int32
    dma = pltpu.SemaphoreType.DMA
    scratch = [
        pltpu.VMEM((ROWS, DIM), bf16), pltpu.VMEM((2, TOP_K, SEQ), i32), pltpu.VMEM((2, TOP_K, SEQ), i32), pltpu.VMEM((2, TOP_K, SEQ), bf16),
        pltpu.VMEM((DIM,), bf16), pltpu.VMEM((DIM,), bf16),
        pltpu.VMEM((LOCAL * FFN, DIM), bf16), pltpu.VMEM((DIM, DIM), bf16), pltpu.VMEM((LOCAL, DIM, FFN), bf16), pltpu.VMEM((LOCAL, DIM, FFN), bf16),
        pltpu.VMEM((NQ, ROWS, QCH), bf16), pltpu.VMEM((ROWS, DIM), bf16), pltpu.VMEM((GROUP, ROWS, DIM), bf16),
        pltpu.VMEM((GROUP, 2, TOP_K, SEQ), i32), pltpu.VMEM((GROUP, 2, TOP_K, SEQ), f32),
        pltpu.VMEM((GROUP, RROWS, ROWS), bf16), pltpu.VMEM((GROUP, ROWS, RROWS), bf16),
        pltpu.VMEM((GROUP, LOCAL, 2 * SLOTS, DIM), bf16), pltpu.VMEM((GROUP, LOCAL, 2 * SLOTS, FFN), bf16), pltpu.VMEM((2, GROUP, LOCAL, 2 * SLOTS, NB), bf16),
        pltpu.VMEM((NBLK, 2, ROWS, NB), f32), pltpu.VMEM((NBLK, 2, ROWS, NB), f32), pltpu.VMEM((NBLK, ROWS, NB), f32), pltpu.VMEM((NBLK, ROWS, NB), f32),
        pltpu.VMEM((ROWS, DIM), f32), pltpu.VMEM((ROWS, DIM), bf16), pltpu.VMEM((LOCAL, 2, EROWS, FFN), f32),
        dma((10,)), dma((NQ,)), dma((1,)), dma((2, len(KS))), dma((NBLK,)), dma((1,)),
        dma((2, 3)), dma((2, 3)), dma((len(KS), 3)), dma((len(KS), 3)), dma((NBLK, 2)), dma((NBLK, 2)), dma((NBLK,)), dma((NBLK,)),
    ]
    both = pl.pallas_call(
        layer_kernel,
        out_shape=jax.ShapeDtypeStruct((ROWS, DIM), bf16),
        in_specs=[pl.BlockSpec(memory_space=pl.ANY)] * len(operands),
        out_specs=pl.BlockSpec(memory_space=pl.ANY),
        scratch_shapes=scratch,
        compiler_params=pltpu.CompilerParams(collective_id=0, has_side_effects=True, vmem_limit_bytes=VMEM_LIMIT),
        name="moe_layer",
    )(*operands)
    return split(both)


def split_kernel(both, out_a, out_b, sem):
    copies = [pltpu.make_async_copy(both.at[pl.ds(i * SEQ, SEQ)], dst, sem.at[i]) for i, dst in enumerate((out_a, out_b))]
    for cp in copies:
        cp.start()
    for cp in copies:
        cp.wait()


def split(both):
    shape = jax.ShapeDtypeStruct((SEQ, DIM), jnp.bfloat16)
    return pl.pallas_call(
        split_kernel,
        out_shape=(shape, shape),
        in_specs=[pl.BlockSpec(memory_space=pltpu.VMEM)],
        out_specs=[pl.BlockSpec(memory_space=pl.ANY)] * 2,
        scratch_shapes=[pltpu.SemaphoreType.DMA((2,))],
        name="split",
    )(both)


def solution(mesh):
    row_spec = P(("dp", "ep"), None)
    full_spec = P(None, None, None)
    gain_spec = P(None)
    expert_spec = P("ep", None, None)
    in_specs = (row_spec, row_spec, row_spec, row_spec, row_spec, row_spec, row_spec, row_spec, gain_spec, full_spec, full_spec, full_spec, full_spec, gain_spec, expert_spec, expert_spec, expert_spec)
    return jax.shard_map(device_fn, mesh=mesh, in_specs=in_specs, out_specs=(row_spec, row_spec), check_vma=False)
```

```python
import functools

import jax
import jax.numpy as jnp
from jax import lax
from jax.experimental import pallas as pl
from jax.experimental.pallas import tpu as pltpu
from jax.sharding import PartitionSpec as P

NORM_EPS = 1e-6
MASK_VALUE = -1e30
MESH = pl.DeviceIdType.MESH
VMEM_LIMIT = 66_000_000

SEQ = 32
ROWS = 2 * SEQ
TOP_K = 8
DIM = 1536
HEAD = 64
FFN = 512
SLOTS = 8
LOCAL = 10
EXPERTS = 40
GROUP = 4
TOKENS = GROUP * ROWS
EROWS = GROUP * 2 * SLOTS
RROWS = LOCAL * 2 * SLOTS
KS = (256, 256, 512, 512)
KOFF = tuple(sum(KS[:k]) for k in range(len(KS)))
NBS = (128, 256, 256, 256, 256, 256, 128)
NOFF = tuple(sum(NBS[:n]) for n in range(len(NBS)))
NBLK = len(NBS)
QCH = 512
PER = DIM // QCH
NQ = 3 * PER

NT = (((1,), (1,)), ((), ()))
NN = (((1,), (0,)), ((), ()))


def dot(lhs, rhs, dims=NN):
    return lax.dot_general(lhs, rhs, dims, preferred_element_type=jnp.float32)


def rms_norm(rows_f, gain):
    inv_rms = lax.rsqrt(jnp.mean(rows_f * rows_f, axis=-1, keepdims=True) + NORM_EPS)
    return (rows_f * inv_rms * gain).astype(jnp.bfloat16)


def layer_kernel(
    tok_a, exp_a, slot_a, gate_a, tok_b, exp_b, slot_b, gate_b, again_h, mgain_h, wq, wk, wv, wo, wg, wu, wd,
    out_h,
    x_v, exp_v, slot_v, gate_v, again, mgain, buf1, wo_v, wg_v, wu_v, qkv, ctx, u_all, codes, gts, disp, comb_t, xg, hid, o_v,
    p_send, p_recv, s_send, r_recv, keep, out_v, acc,
    in_sem, q_sem, o_sem, g_sem, d_sem, out_sem, c_send, c_recv, u_send, u_recv, ps_sem, pr_sem, ss_sem, rr_sem,
):
    me = lax.axis_index("ep")
    dp = lax.axis_index("dp")
    x_pos = me // 2
    core = lax.rem(me, 2)
    sib = (dp, x_pos * 2 + (1 - core))
    cross = (dp, (1 - x_pos) * 2 + core)

    ins = []
    for i, (src, dst) in enumerate([
        (tok_a, x_v.at[pl.ds(0, SEQ)]), (tok_b, x_v.at[pl.ds(SEQ, SEQ)]), (again_h, again),
        (exp_a, exp_v.at[0]), (exp_b, exp_v.at[1]), (slot_a, slot_v.at[0]), (slot_b, slot_v.at[1]),
        (gate_a, gate_v.at[0]), (gate_b, gate_v.at[1]), (mgain_h, mgain),
    ]):
        cp = pltpu.make_async_copy(src, dst, in_sem.at[i])
        cp.start()
        ins.append(cp)

    q_cp = []
    for i in range(NQ):
        w, r = (wq, wk, wv)[i // PER], i % PER
        cp = pltpu.make_async_copy(w.at[pl.ds(r * QCH, QCH)], buf1.at[pl.ds(i * QCH, QCH)], q_sem.at[i])
        cp.start(priority=1)
        q_cp.append(cp)
    o_cp = pltpu.make_async_copy(wo, wo_v, o_sem.at[0])
    o_cp.start(priority=1)

    g_cp = []
    for k, (off, size) in enumerate(zip(KOFF, KS)):
        ks = pl.ds(off, size)
        g_cp.append([pltpu.make_async_copy(w.at[:, ks, :], v.at[:, ks, :], g_sem.at[i, k]) for i, (w, v) in enumerate(((wg, wg_v), (wu, wu_v)))])

    def fetch(k):
        for cp in g_cp[k]:
            cp.start(priority=1)

    barrier = pltpu.get_barrier_semaphore()
    for peer in (sib, cross):
        pl.semaphore_signal(barrier, inc=1, device_id=peer, device_id_type=MESH)

    for cp in ins:
        cp.wait()

    for b in range(2):
        s = slot_v[b]
        codes[0, b] = jnp.where(s >= 0, exp_v[b] * SLOTS + s, -1)
        gts[0, b] = gate_v[b].astype(jnp.float32)

    def remote(src, dst, ssem, rsem, dev):
        return pltpu.make_async_remote_copy(src_ref=src, dst_ref=dst, send_sem=ssem, recv_sem=rsem, device_id=dev, device_id_type=MESH)

    def exchange(buf, ssem, rsem):
        to_cross = remote(buf.at[0], buf.at[1], ssem.at[0], rsem.at[0], cross)
        to_sib = remote(buf.at[0], buf.at[2], ssem.at[1], rsem.at[1], sib)
        relay = remote(buf.at[1], buf.at[3], ssem.at[2], rsem.at[2], sib)
        return to_cross, to_sib, relay

    x_f = x_v[...].astype(jnp.float32)
    normed = rms_norm(x_f, again[...].astype(jnp.float32).reshape(1, DIM))

    def project(first, last):
        rows = pl.ds(first * QCH, (last - first) * QCH)
        res = dot(normed, buf1[rows, :], NT).astype(jnp.bfloat16)
        for i in range(first, last):
            qkv[i] = res[:, (i - first) * QCH:(i - first + 1) * QCH]

    q_cp[0].wait()
    fetch(0)
    project(0, 1)
    q_cp[1].wait()
    q_cp[2].wait()
    fetch(1)
    project(1, 3)

    for i in (3, 4, 5):
        q_cp[i].wait()
    fetch(2)
    project(3, 6)

    pl.semaphore_wait(barrier, 2)
    c_copies = exchange(codes, c_send.at[0], c_recv.at[0])
    g_copies = exchange(gts, c_send.at[1], c_recv.at[1])
    for cp in (*c_copies[:2], *g_copies[:2]):
        cp.start()

    for i in (6, 7, 8):
        q_cp[i].wait()
    fetch(3)
    q_row = lax.rem(lax.broadcasted_iota(jnp.int32, (4 * ROWS, ROWS), 0), ROWS)
    k_col = lax.broadcasted_iota(jnp.int32, (4 * ROWS, ROWS), 1)
    seen = (k_col <= q_row) & (k_col // SEQ == q_row // SEQ)
    lane_head = lax.broadcasted_iota(jnp.int32, (ROWS, 4 * HEAD), 1) // HEAD
    groups = QCH // 256
    probs = []
    for g in range(DIM // 256):
        part = pl.ds((g % groups) * 256, 256)
        q4 = qkv[g // groups, :, part]
        k4 = qkv[PER + g // groups, :, part]
        zero = jnp.zeros_like(q4)
        q_blocks = jnp.concatenate([jnp.where(lane_head == h, q4, zero) for h in range(4)], axis=0)
        s = dot(q_blocks, k4, NT) * (HEAD ** -0.5)
        s = jnp.where(seen, s, MASK_VALUE)
        ex = jnp.exp(s - jnp.max(s, axis=-1, keepdims=True))
        probs.append((ex / jnp.sum(ex, axis=-1, keepdims=True)).astype(jnp.bfloat16))
    project(6, 9)
    o_cp.wait()
    for g in range(DIM // 256):
        v4 = qkv[2 * PER + g // groups, :, pl.ds((g % groups) * 256, 256)]
        mixed = dot(probs[g], v4)
        c4 = mixed[0:ROWS]
        for h in range(1, 4):
            c4 = jnp.where(lane_head == h, mixed[h * ROWS:(h + 1) * ROWS], c4)
        ctx[:, pl.ds(g * 256, 256)] = c4.astype(jnp.bfloat16)

    h = (x_f + dot(ctx[...], wo_v[...])).astype(jnp.bfloat16)
    keep[...] = h.astype(jnp.float32)
    u_all[0] = rms_norm(h.astype(jnp.float32), mgain[...].astype(jnp.float32).reshape(1, DIM))

    u_copies = []
    for k, (off, size) in enumerate(zip(KOFF, KS)):
        view = u_all.at[:, :, pl.ds(off, size)]
        u_copies.append(exchange(view, u_send.at[k], u_recv.at[k]))
        u_copies[k][0].start()
    for copies in u_copies:
        copies[1].start()

    d_cp = []
    for n in range(NBLK):
        cols = pl.ds(NOFF[n], NBS[n])
        cp = pltpu.make_async_copy(wd.at[:, cols], buf1.at[:, cols], d_sem.at[n])
        cp.start(priority=1)
        d_cp.append(cp)

    c_copies[0].wait_recv()
    c_copies[2].start()
    g_copies[0].wait_recv()
    g_copies[2].start()
    for cp in (c_copies[1], g_copies[1], c_copies[2], g_copies[2]):
        cp.wait_recv()
    row = lax.broadcasted_iota(jnp.int32, (RROWS, ROWS), 0)
    want = (row // (2 * SLOTS) + me * LOCAL) * SLOTS + lax.rem(row, SLOTS) + lax.rem(row // SLOTS, 2) * (EXPERTS * SLOTS)
    for r in range(GROUP):
        code = jnp.concatenate([codes[r, 0], jnp.where(codes[r, 1] >= 0, codes[r, 1] + EXPERTS * SLOTS, -1)], axis=1)
        gate = jnp.concatenate([gts[r, 0], gts[r, 1]], axis=1)
        val = jnp.zeros((RROWS, ROWS), jnp.float32)
        hit = jnp.zeros((RROWS, ROWS), jnp.float32)
        for j in range(TOP_K):
            same = jnp.broadcast_to(code[j:j + 1, :], (RROWS, ROWS)) == want
            val = jnp.where(same, jnp.broadcast_to(gate[j:j + 1, :], (RROWS, ROWS)), val)
            hit = jnp.where(same, 1.0, hit)
        disp[r] = hit.astype(jnp.bfloat16)
        comb_t[r] = val.T.astype(jnp.bfloat16)

    def gather(r, k):
        ks = pl.ds(KOFF[k], KS[k])
        xg[r, :, :, ks] = dot(disp[r], u_all[r, :, ks]).astype(jnp.bfloat16).reshape(LOCAL, 2 * SLOTS, KS[k])

    for k in range(len(KS)):
        gather(0, k)
    for k in range(len(KS)):
        u_copies[k][1].wait_recv()
    for k in range(len(KS)):
        gather(2, k)

    def relay(k):
        u_copies[k][0].wait_recv()
        u_copies[k][2].start()

    def experts(k, first, last):
        ks = pl.ds(KOFF[k], KS[k])
        for e in range(first, last):
            xe = xg[:, e, :, ks].reshape(EROWS, KS[k])
            gate_act = dot(xe, wg_v[e, ks, :])
            up_act = dot(xe, wu_v[e, ks, :])
            if k > 0:
                gate_act = acc[e, 0] + gate_act
                up_act = acc[e, 1] + up_act
            if k + 1 < len(KS):
                acc[e, 0] = gate_act
                acc[e, 1] = up_act
            else:
                hid[:, e] = (jax.nn.silu(gate_act) * up_act).astype(jnp.bfloat16).reshape(GROUP, 2 * SLOTS, FFN)

    relay(0)
    gather(1, 0)
    relay(1)
    gather(1, 1)
    for k in range(len(KS)):
        if k == 1:
            relay(2)
            gather(1, 2)
        u_copies[k][2].wait_recv()
        for cp in g_cp[k]:
            cp.wait()
        gather(3, k)
        half = LOCAL // 2
        experts(k, 0, half)
        if k == 2:
            relay(3)
            gather(1, 3)
        experts(k, half, LOCAL)

    cols = [pl.ds(NOFF[n], NBS[n]) for n in range(NBLK)]
    to_sib = [[remote(p_send.at[i, :, c], p_recv.at[i, :, c], ps_sem.at[n, i], pr_sem.at[n, i], sib) for i in range(2)] for n, c in enumerate(cols)]
    to_cross = [remote(s_send.at[:, c], r_recv.at[:, c], ss_sem.at[n], rr_sem.at[n], cross) for n, c in enumerate(cols)]

    def forward(n):
        to_sib[n][1].wait_recv()
        s_send[:, cols[n]] = s_send[:, cols[n]] + p_recv[1, :, cols[n]]
        to_cross[n].start()

    def down(n):
        for e in range(LOCAL):
            res = dot(hid[:, e].reshape(EROWS, FFN), buf1[pl.ds(e * FFN, FFN), cols[n]])
            o_v[n % 2, :, e, :, pl.ds(0, NBS[n])] = res.astype(jnp.bfloat16).reshape(GROUP, 2 * SLOTS, NBS[n])

    def combine(n, r):
        return dot(comb_t[r], o_v[n % 2, r, :, :, pl.ds(0, NBS[n])].reshape(RROWS, NBS[n]))

    d_cp[0].wait()
    down(0)
    p_send[1, :, cols[0]] = combine(0, 3)
    to_sib[0][1].start()
    for n in range(NBLK):
        if n + 1 < NBLK:
            d_cp[n + 1].wait()
        if n > 0:
            p_send[1, :, cols[n]] = combine(n, 3)
        s_send[:, cols[n]] = combine(n, 1)
        p_send[0, :, cols[n]] = combine(n, 2)
        keep[:, cols[n]] = keep[:, cols[n]] + combine(n, 0)
        if n + 1 < NBLK:
            down(n + 1)
        if n > 0:
            to_sib[n][1].start()
        to_sib[n][0].start()
        if n > 1:
            forward(n - 1)
        if n == 0:
            forward(0)
    forward(NBLK - 1)

    for n in range(NBLK):
        to_sib[n][0].wait_recv()
        to_cross[n].wait_recv()
        out_v[:, cols[n]] = (keep[:, cols[n]] + p_recv[0, :, cols[n]] + r_recv[:, cols[n]]).astype(jnp.bfloat16)

    out_cp = pltpu.make_async_copy(out_v, out_h, out_sem.at[0])
    out_cp.start()
    for cp in (*c_copies, *g_copies, *(c for cs in u_copies for c in cs), *(c for cs in to_sib for c in cs), *to_cross):
        cp.wait_send()
    out_cp.wait()


def device_fn(tokens_a, experts_a, slots_a, gates_a, tokens_b, experts_b, slots_b, gates_b, attn_gain, w_query, w_key, w_value, w_out, moe_gain, w_gate, w_up, w_down):
    def by_row(w):
        return jnp.transpose(w, (1, 2, 0)).reshape(DIM, DIM)

    operands = (
        tokens_a, experts_a.T, slots_a.T, gates_a.T, tokens_b, experts_b.T, slots_b.T, gates_b.T, attn_gain, moe_gain,
        by_row(w_query), by_row(w_key), by_row(w_value), w_out.reshape(DIM, DIM), w_gate, w_up, w_down.reshape(LOCAL * FFN, DIM),
    )
    bf16, f32, i32 = jnp.bfloat16, jnp.float32, jnp.int32
    dma = pltpu.SemaphoreType.DMA
    scratch = [
        pltpu.VMEM((ROWS, DIM), bf16), pltpu.VMEM((2, TOP_K, SEQ), i32), pltpu.VMEM((2, TOP_K, SEQ), i32), pltpu.VMEM((2, TOP_K, SEQ), bf16),
        pltpu.VMEM((DIM,), bf16), pltpu.VMEM((DIM,), bf16),
        pltpu.VMEM((LOCAL * FFN, DIM), bf16), pltpu.VMEM((DIM, DIM), bf16), pltpu.VMEM((LOCAL, DIM, FFN), bf16), pltpu.VMEM((LOCAL, DIM, FFN), bf16),
        pltpu.VMEM((NQ, ROWS, QCH), bf16), pltpu.VMEM((ROWS, DIM), bf16), pltpu.VMEM((GROUP, ROWS, DIM), bf16),
        pltpu.VMEM((GROUP, 2, TOP_K, SEQ), i32), pltpu.VMEM((GROUP, 2, TOP_K, SEQ), f32),
        pltpu.VMEM((GROUP, RROWS, ROWS), bf16), pltpu.VMEM((GROUP, ROWS, RROWS), bf16),
        pltpu.VMEM((GROUP, LOCAL, 2 * SLOTS, DIM), bf16), pltpu.VMEM((GROUP, LOCAL, 2 * SLOTS, FFN), bf16), pltpu.VMEM((2, GROUP, LOCAL, 2 * SLOTS, max(NBS)), bf16),
        pltpu.VMEM((2, ROWS, DIM), f32), pltpu.VMEM((2, ROWS, DIM), f32), pltpu.VMEM((ROWS, DIM), f32), pltpu.VMEM((ROWS, DIM), f32),
        pltpu.VMEM((ROWS, DIM), f32), pltpu.VMEM((ROWS, DIM), bf16), pltpu.VMEM((LOCAL, 2, EROWS, FFN), f32),
        dma((10,)), dma((NQ,)), dma((1,)), dma((2, len(KS))), dma((NBLK,)), dma((1,)),
        dma((2, 3)), dma((2, 3)), dma((len(KS), 3)), dma((len(KS), 3)), dma((NBLK, 2)), dma((NBLK, 2)), dma((NBLK,)), dma((NBLK,)),
    ]
    both = pl.pallas_call(
        layer_kernel,
        out_shape=jax.ShapeDtypeStruct((ROWS, DIM), bf16),
        in_specs=[pl.BlockSpec(memory_space=pl.ANY)] * len(operands),
        out_specs=pl.BlockSpec(memory_space=pl.ANY),
        scratch_shapes=scratch,
        compiler_params=pltpu.CompilerParams(collective_id=0, has_side_effects=True, vmem_limit_bytes=VMEM_LIMIT),
        name="moe_layer",
    )(*operands)
    return split(both)


def split_kernel(both, out_a, out_b, sem):
    copies = [pltpu.make_async_copy(both.at[pl.ds(i * SEQ, SEQ)], dst, sem.at[i]) for i, dst in enumerate((out_a, out_b))]
    for cp in copies:
        cp.start()
    for cp in copies:
        cp.wait()


def split(both):
    shape = jax.ShapeDtypeStruct((SEQ, DIM), jnp.bfloat16)
    return pl.pallas_call(
        split_kernel,
        out_shape=(shape, shape),
        in_specs=[pl.BlockSpec(memory_space=pltpu.VMEM)],
        out_specs=[pl.BlockSpec(memory_space=pl.ANY)] * 2,
        scratch_shapes=[pltpu.SemaphoreType.DMA((2,))],
        name="split",
    )(both)


def solution(mesh):
    row_spec = P(("dp", "ep"), None)
    full_spec = P(None, None, None)
    gain_spec = P(None)
    expert_spec = P("ep", None, None)
    in_specs = (row_spec, row_spec, row_spec, row_spec, row_spec, row_spec, row_spec, row_spec, gain_spec, full_spec, full_spec, full_spec, full_spec, gain_spec, expert_spec, expert_spec, expert_spec)
    return jax.shard_map(device_fn, mesh=mesh, in_specs=in_specs, out_specs=(row_spec, row_spec), check_vma=False)
```

```python
import functools

import jax
import jax.numpy as jnp
from jax import lax
from jax.experimental import pallas as pl
from jax.experimental.pallas import tpu as pltpu
from jax.sharding import PartitionSpec as P

NORM_EPS = 1e-6
MASK_VALUE = -1e30
MESH = pl.DeviceIdType.MESH
VMEM_LIMIT = 53_000_000

SEQ = 32
ROWS = 2 * SEQ
TOP_K = 8
DIM = 1536
HEAD = 64
FFN = 512
SLOTS = 8
LOCAL = 10
EXPERTS = 40
GROUP = 4
TOKENS = GROUP * ROWS
EROWS = GROUP * 2 * SLOTS
RROWS = LOCAL * 2 * SLOTS
KS = (256, 256, 512, 512)
KOFF = tuple(sum(KS[:k]) for k in range(len(KS)))
NBS = (256, 256, 256, 256, 256, 256)
NOFF = tuple(sum(NBS[:n]) for n in range(len(NBS)))
NBLK = len(NBS)
QCH = 512
PER = DIM // QCH
NQ = 3 * PER

BLK = 512
PIECES = DIM // BLK
X0, W0, Y0, Z0 = 0, 27, 36, 56
POOL = 76
KWHERE = ((Y0, 0), (Y0, 256), (Z0, 0), (X0, 0))
DOWN = (
    tuple(X0 + 20 + e for e in range(7)) + tuple(W0 + e for e in range(3)),
    tuple(W0 + 3 + e for e in range(6)) + tuple(Y0 + e for e in range(4)),
    tuple(Y0 + 4 + e for e in range(10)),
)

NT = (((1,), (1,)), ((), ()))
NN = (((1,), (0,)), ((), ()))


def dot(lhs, rhs, dims=NN):
    return lax.dot_general(lhs, rhs, dims, preferred_element_type=jnp.float32)


def rms_norm(rows_f, gain):
    inv_rms = lax.rsqrt(jnp.mean(rows_f * rows_f, axis=-1, keepdims=True) + NORM_EPS)
    return (rows_f * inv_rms * gain).astype(jnp.bfloat16)


def layer_kernel(
    tok_a, exp_a, slot_a, gate_a, tok_b, exp_b, slot_b, gate_b, again_h, mgain_h, wq, wk, wv, wo, wg, wu, wd,
    out_h,
    x_v, exp_v, slot_v, gate_v, again, mgain, pool, qkv, ctx, u_all, codes, gts, disp, comb_t, xg, hid, o_v,
    p_send, p_recv, s_send, r_recv, keep, acc,
    in_sem, q_sem, o_sem, g_sem, d_sem, c_send, c_recv, u_send, u_recv, ps_sem, pr_sem, ss_sem, rr_sem,
):
    me = lax.axis_index("ep")
    dp = lax.axis_index("dp")
    x_pos = me // 2
    core = lax.rem(me, 2)
    sib = (dp, x_pos * 2 + (1 - core))
    cross = (dp, (1 - x_pos) * 2 + core)

    ins = []
    for i, (src, dst) in enumerate([
        (tok_a, x_v.at[pl.ds(0, SEQ)]), (tok_b, x_v.at[pl.ds(SEQ, SEQ)]), (again_h, again),
        (exp_a, exp_v.at[0]), (exp_b, exp_v.at[1]), (slot_a, slot_v.at[0]), (slot_b, slot_v.at[1]),
        (gate_a, gate_v.at[0]), (gate_b, gate_v.at[1]), (mgain_h, mgain),
    ]):
        cp = pltpu.make_async_copy(src, dst, in_sem.at[i])
        cp.start()
        ins.append(cp)

    q_cp = []
    for i, (w, first, last) in enumerate(((wq, 0, 1), (wq, 1, 3), (wk, 0, 3), (wv, 0, 3))):
        base = X0 + (0, 0, 3, 6)[i] + first
        q_cp.append([
            pltpu.make_async_copy(w.at[pl.ds(first, last - first), :, pl.ds(c * BLK, BLK)], pool.at[pl.ds(base + 9 * c, last - first)], q_sem.at[i, c])
            for c in range(PIECES)
        ])
        for cp in q_cp[i]:
            cp.start(priority=1)
    o_cp = [pltpu.make_async_copy(wo.at[:, :, pl.ds(c * BLK, BLK)], pool.at[pl.ds(W0 + 3 * c, 3)], o_sem.at[c]) for c in range(PIECES)]
    for cp in o_cp:
        cp.start(priority=1)

    g_cp = []
    for k, (off, size) in enumerate(zip(KOFF, KS)):
        base, row = KWHERE[k]
        g_cp.append([
            pltpu.make_async_copy(w.at[:, pl.ds(off, size), :], pool.at[pl.ds(base + LOCAL * i, LOCAL), pl.ds(row, size), :], g_sem.at[i, k])
            for i, w in enumerate((wg, wu))
        ])

    def fetch(k):
        for cp in g_cp[k]:
            cp.start(priority=1)

    d_cp = []
    for p, (first, last) in ((0, (0, 7)), (0, (7, 10)), (1, (0, 6)), (1, (6, 10)), (2, (0, 10))):
        src = wd.at[pl.ds(first, last - first), :, pl.ds(p * BLK, BLK)]
        d_cp.append(pltpu.make_async_copy(src, pool.at[pl.ds(DOWN[p][first], last - first)], d_sem.at[len(d_cp)]))

    barrier = pltpu.get_barrier_semaphore()
    for peer in (sib, cross):
        pl.semaphore_signal(barrier, inc=1, device_id=peer, device_id_type=MESH)

    for cp in ins:
        cp.wait()

    for b in range(2):
        s = slot_v[b]
        codes[0, b] = jnp.where(s >= 0, exp_v[b] * SLOTS + s, -1)
        gts[0, b] = gate_v[b].astype(jnp.float32)

    def remote(src, dst, ssem, rsem, dev):
        return pltpu.make_async_remote_copy(src_ref=src, dst_ref=dst, send_sem=ssem, recv_sem=rsem, device_id=dev, device_id_type=MESH)

    def exchange(buf, ssem, rsem):
        to_cross = remote(buf.at[0], buf.at[1], ssem.at[0], rsem.at[0], cross)
        to_sib = remote(buf.at[0], buf.at[2], ssem.at[1], rsem.at[1], sib)
        relay = remote(buf.at[1], buf.at[3], ssem.at[2], rsem.at[2], sib)
        return to_cross, to_sib, relay

    x_f = x_v[...].astype(jnp.float32)
    normed = rms_norm(x_f, again[...].astype(jnp.float32).reshape(1, DIM))

    def project(first, last):
        for i in range(first, last):
            res = sum(dot(normed[:, c * BLK:(c + 1) * BLK], pool[X0 + 9 * c + i], NT) for c in range(PIECES))
            qkv[i] = res.astype(jnp.bfloat16)

    def arrived(copies):
        for cp in copies:
            cp.wait()

    arrived(q_cp[0])
    fetch(0)
    project(0, 1)
    arrived(q_cp[1])
    fetch(1)
    project(1, 3)

    arrived(q_cp[2])
    fetch(2)
    project(3, 6)

    pl.semaphore_wait(barrier, 2)
    c_copies = exchange(codes, c_send.at[0], c_recv.at[0])
    g_copies = exchange(gts, c_send.at[1], c_recv.at[1])
    for cp in (*c_copies[:2], *g_copies[:2]):
        cp.start()

    arrived(q_cp[3])
    q_row = lax.rem(lax.broadcasted_iota(jnp.int32, (4 * ROWS, ROWS), 0), ROWS)
    k_col = lax.broadcasted_iota(jnp.int32, (4 * ROWS, ROWS), 1)
    seen = (k_col <= q_row) & (k_col // SEQ == q_row // SEQ)
    lane_head = lax.broadcasted_iota(jnp.int32, (ROWS, 4 * HEAD), 1) // HEAD
    groups = QCH // 256
    probs = []
    for g in range(DIM // 256):
        part = pl.ds((g % groups) * 256, 256)
        q4 = qkv[g // groups, :, part]
        k4 = qkv[PER + g // groups, :, part]
        zero = jnp.zeros_like(q4)
        q_blocks = jnp.concatenate([jnp.where(lane_head == h, q4, zero) for h in range(4)], axis=0)
        s = dot(q_blocks, k4, NT) * (HEAD ** -0.5)
        s = jnp.where(seen, s, MASK_VALUE)
        ex = jnp.exp(s - jnp.max(s, axis=-1, keepdims=True))
        probs.append((ex / jnp.sum(ex, axis=-1, keepdims=True)).astype(jnp.bfloat16))
    project(6, 9)
    fetch(3)
    arrived(o_cp)
    for g in range(DIM // 256):
        v4 = qkv[2 * PER + g // groups, :, pl.ds((g % groups) * 256, 256)]
        mixed = dot(probs[g], v4)
        c4 = mixed[0:ROWS]
        for h in range(1, 4):
            c4 = jnp.where(lane_head == h, mixed[h * ROWS:(h + 1) * ROWS], c4)
        ctx[:, pl.ds(g * 256, 256)] = c4.astype(jnp.bfloat16)

    mixed_in = ctx[...]
    attn_out = [sum(dot(mixed_in[:, i * BLK:(i + 1) * BLK], pool[W0 + 3 * c + i]) for i in range(3)) for c in range(PIECES)]
    h = (x_f + jnp.concatenate(attn_out, axis=1)).astype(jnp.bfloat16)
    keep[...] = h.astype(jnp.float32)
    u_all[0] = rms_norm(h.astype(jnp.float32), mgain[...].astype(jnp.float32).reshape(1, DIM))

    u_copies = []
    for k, (off, size) in enumerate(zip(KOFF, KS)):
        view = u_all.at[:, :, pl.ds(off, size)]
        u_copies.append(exchange(view, u_send.at[k], u_recv.at[k]))
        u_copies[k][0].start()
    for copies in u_copies:
        copies[1].start()

    for cp in d_cp[:3]:
        cp.start(priority=1)

    c_copies[0].wait_recv()
    c_copies[2].start()
    g_copies[0].wait_recv()
    g_copies[2].start()
    for cp in (c_copies[1], g_copies[1], c_copies[2], g_copies[2]):
        cp.wait_recv()
    row = lax.broadcasted_iota(jnp.int32, (RROWS, ROWS), 0)
    want = (row // (2 * SLOTS) + me * LOCAL) * SLOTS + lax.rem(row, SLOTS) + lax.rem(row // SLOTS, 2) * (EXPERTS * SLOTS)
    for r in range(GROUP):
        code = jnp.concatenate([codes[r, 0], jnp.where(codes[r, 1] >= 0, codes[r, 1] + EXPERTS * SLOTS, -1)], axis=1)
        gate = jnp.concatenate([gts[r, 0], gts[r, 1]], axis=1)
        val = jnp.zeros((RROWS, ROWS), jnp.float32)
        hit = jnp.zeros((RROWS, ROWS), jnp.float32)
        for j in range(TOP_K):
            same = jnp.broadcast_to(code[j:j + 1, :], (RROWS, ROWS)) == want
            val = jnp.where(same, jnp.broadcast_to(gate[j:j + 1, :], (RROWS, ROWS)), val)
            hit = jnp.where(same, 1.0, hit)
        disp[r] = hit.astype(jnp.bfloat16)
        comb_t[r] = val.T.astype(jnp.bfloat16)

    def gather(r, k):
        ks = pl.ds(KOFF[k], KS[k])
        xg[r, :, :, ks] = dot(disp[r], u_all[r, :, ks]).astype(jnp.bfloat16).reshape(LOCAL, 2 * SLOTS, KS[k])

    for k in range(len(KS)):
        gather(0, k)
    for k in range(len(KS)):
        u_copies[k][1].wait_recv()
    for k in range(len(KS)):
        gather(2, k)

    def relay(k):
        u_copies[k][0].wait_recv()
        u_copies[k][2].start()

    def experts(k, first, last):
        ks = pl.ds(KOFF[k], KS[k])
        for e in range(first, last):
            xe = xg[:, e, :, ks].reshape(EROWS, KS[k])
            base, row = KWHERE[k]
            rows = pl.ds(row, KS[k])
            gate_act = dot(xe, pool[base + e, rows, :])
            up_act = dot(xe, pool[base + LOCAL + e, rows, :])
            if k > 0:
                gate_act = acc[e, 0] + gate_act
                up_act = acc[e, 1] + up_act
            if k + 1 < len(KS):
                acc[e, 0] = gate_act
                acc[e, 1] = up_act
            else:
                hid[:, e] = (jax.nn.silu(gate_act) * up_act).astype(jnp.bfloat16).reshape(GROUP, 2 * SLOTS, FFN)

    relay(0)
    gather(1, 0)
    relay(1)
    gather(1, 1)
    for k in range(len(KS)):
        if k == 1:
            relay(2)
            gather(1, 2)
        u_copies[k][2].wait_recv()
        for cp in g_cp[k]:
            cp.wait()
        gather(3, k)
        half = LOCAL // 2
        experts(k, 0, half)
        if k == 2:
            relay(3)
            gather(1, 3)
        experts(k, half, LOCAL)
        if k == 1:
            for cp in d_cp[3:]:
                cp.start(priority=1)

    cols = [pl.ds(NOFF[n], NBS[n]) for n in range(NBLK)]
    to_sib = [[remote(p_send.at[i, :, c], p_recv.at[i, :, c], ps_sem.at[n, i], pr_sem.at[n, i], sib) for i in range(2)] for n, c in enumerate(cols)]
    to_cross = [remote(s_send.at[:, c], r_recv.at[:, c], ss_sem.at[n], rr_sem.at[n], cross) for n, c in enumerate(cols)]

    def forward(n):
        to_sib[n][1].wait_recv()
        s_send[:, cols[n]] = s_send[:, cols[n]] + p_recv[1, :, cols[n]]
        to_cross[n].start()

    def down(n):
        p, off = NOFF[n] // BLK, NOFF[n] % BLK
        for e in range(LOCAL):
            res = dot(hid[:, e].reshape(EROWS, FFN), pool[DOWN[p][e], :, pl.ds(off, NBS[n])])
            o_v[n % 2, :, e, :, pl.ds(0, NBS[n])] = res.astype(jnp.bfloat16).reshape(GROUP, 2 * SLOTS, NBS[n])

    def combine(n, r):
        return dot(comb_t[r], o_v[n % 2, r, :, :, pl.ds(0, NBS[n])].reshape(RROWS, NBS[n]))

    arrived(d_cp[:2])
    down(0)
    p_send[1, :, cols[0]] = combine(0, 3)
    to_sib[0][1].start()
    for n in range(NBLK):
        if n + 1 < NBLK and NOFF[n + 1] == BLK:
            arrived(d_cp[2:4])
        if n + 1 < NBLK and NOFF[n + 1] == 2 * BLK:
            arrived(d_cp[4:])
        if n > 0:
            p_send[1, :, cols[n]] = combine(n, 3)
        s_send[:, cols[n]] = combine(n, 1)
        p_send[0, :, cols[n]] = combine(n, 2)
        keep[:, cols[n]] = keep[:, cols[n]] + combine(n, 0)
        if n + 1 < NBLK:
            down(n + 1)
        if n > 0:
            to_sib[n][1].start()
        to_sib[n][0].start()
        if n > 1:
            forward(n - 1)
        if n == 0:
            forward(0)
    forward(NBLK - 1)

    for n in range(NBLK):
        to_sib[n][0].wait_recv()
        to_cross[n].wait_recv()
        out_h[:, cols[n]] = (keep[:, cols[n]] + p_recv[0, :, cols[n]] + r_recv[:, cols[n]]).astype(jnp.bfloat16)

    for cp in (*c_copies, *g_copies, *(c for cs in u_copies for c in cs), *(c for cs in to_sib for c in cs), *to_cross):
        cp.wait_send()


def device_fn(tokens_a, experts_a, slots_a, gates_a, tokens_b, experts_b, slots_b, gates_b, attn_gain, w_query, w_key, w_value, w_out, moe_gain, w_gate, w_up, w_down):
    def by_row(w):
        return jnp.transpose(w, (1, 2, 0)).reshape(3, BLK, DIM)

    operands = (
        tokens_a, experts_a.T, slots_a.T, gates_a.T, tokens_b, experts_b.T, slots_b.T, gates_b.T, attn_gain, moe_gain,
        by_row(w_query), by_row(w_key), by_row(w_value), w_out.reshape(3, BLK, DIM), w_gate, w_up, w_down,
    )
    operands = tuple(pltpu.with_memory_space_constraint(x, pltpu.HBM) for x in operands)
    bf16, f32, i32 = jnp.bfloat16, jnp.float32, jnp.int32
    dma = pltpu.SemaphoreType.DMA
    scratch = [
        pltpu.VMEM((ROWS, DIM), bf16), pltpu.VMEM((2, TOP_K, SEQ), i32), pltpu.VMEM((2, TOP_K, SEQ), i32), pltpu.VMEM((2, TOP_K, SEQ), bf16),
        pltpu.VMEM((DIM,), bf16), pltpu.VMEM((DIM,), bf16),
        pltpu.VMEM((POOL, BLK, BLK), bf16),
        pltpu.VMEM((NQ, ROWS, QCH), bf16), pltpu.VMEM((ROWS, DIM), bf16), pltpu.VMEM((GROUP, ROWS, DIM), bf16),
        pltpu.VMEM((GROUP, 2, TOP_K, SEQ), i32), pltpu.VMEM((GROUP, 2, TOP_K, SEQ), f32),
        pltpu.VMEM((GROUP, RROWS, ROWS), bf16), pltpu.VMEM((GROUP, ROWS, RROWS), bf16),
        pltpu.VMEM((GROUP, LOCAL, 2 * SLOTS, DIM), bf16), pltpu.VMEM((GROUP, LOCAL, 2 * SLOTS, FFN), bf16), pltpu.VMEM((2, GROUP, LOCAL, 2 * SLOTS, max(NBS)), bf16),
        pltpu.VMEM((2, ROWS, DIM), f32), pltpu.VMEM((2, ROWS, DIM), f32), pltpu.VMEM((ROWS, DIM), f32), pltpu.VMEM((ROWS, DIM), f32),
        pltpu.VMEM((ROWS, DIM), f32), pltpu.VMEM((LOCAL, 2, EROWS, FFN), f32),
        dma((10,)), dma((4, PIECES)), dma((PIECES,)), dma((2, len(KS))), dma((5,)),
        dma((2, 3)), dma((2, 3)), dma((len(KS), 3)), dma((len(KS), 3)), dma((NBLK, 2)), dma((NBLK, 2)), dma((NBLK,)), dma((NBLK,)),
    ]
    both = pl.pallas_call(
        layer_kernel,
        out_shape=jax.ShapeDtypeStruct((ROWS, DIM), bf16),
        in_specs=[pl.BlockSpec(memory_space=pltpu.HBM)] * len(operands),
        out_specs=pl.BlockSpec(memory_space=pltpu.VMEM),
        scratch_shapes=scratch,
        compiler_params=pltpu.CompilerParams(collective_id=0, has_side_effects=True, vmem_limit_bytes=VMEM_LIMIT),
        name="moe_layer",
    )(*operands)
    return split(both)


def split_kernel(both, out_a, out_b, sem):
    copies = [pltpu.make_async_copy(both.at[pl.ds(i * SEQ, SEQ)], dst, sem.at[i]) for i, dst in enumerate((out_a, out_b))]
    for cp in copies:
        cp.start()
    for cp in copies:
        cp.wait()


def split(both):
    shape = jax.ShapeDtypeStruct((SEQ, DIM), jnp.bfloat16)
    return pl.pallas_call(
        split_kernel,
        out_shape=(shape, shape),
        in_specs=[pl.BlockSpec(memory_space=pl.ANY)],
        out_specs=[pl.BlockSpec(memory_space=pl.ANY)] * 2,
        scratch_shapes=[pltpu.SemaphoreType.DMA((2,))],
        compiler_params=pltpu.CompilerParams(vmem_limit_bytes=1 << 20),
        name="split",
    )(both)


def solution(mesh):
    row_spec = P(("dp", "ep"), None)
    full_spec = P(None, None, None)
    gain_spec = P(None)
    expert_spec = P("ep", None, None)
    in_specs = (row_spec, row_spec, row_spec, row_spec, row_spec, row_spec, row_spec, row_spec, gain_spec, full_spec, full_spec, full_spec, full_spec, gain_spec, expert_spec, expert_spec, expert_spec)
    return jax.shard_map(device_fn, mesh=mesh, in_specs=in_specs, out_specs=(row_spec, row_spec), check_vma=False)
```

```python
import functools

import jax
import jax.numpy as jnp
from jax import lax
from jax.experimental import pallas as pl
from jax.experimental.pallas import tpu as pltpu
from jax.sharding import PartitionSpec as P

NORM_EPS = 1e-6
MASK_VALUE = -1e30
MESH = pl.DeviceIdType.MESH
VMEM_LIMIT = 53_000_000

SEQ = 32
ROWS = 2 * SEQ
TOP_K = 8
DIM = 1536
HEAD = 64
FFN = 512
SLOTS = 8
LOCAL = 10
EXPERTS = 40
GROUP = 4
TOKENS = GROUP * ROWS
EROWS = GROUP * 2 * SLOTS
RROWS = LOCAL * 2 * SLOTS
KS = (256, 256, 512, 512)
KOFF = tuple(sum(KS[:k]) for k in range(len(KS)))
NBS = (256, 256, 256, 256, 256, 256)
NOFF = tuple(sum(NBS[:n]) for n in range(len(NBS)))
NBLK = len(NBS)
QCH = 512
PER = DIM // QCH
NQ = 3 * PER

BLK = 512
PIECES = DIM // BLK
X0, W0, Y0, Z0 = 0, 27, 36, 56
POOL = 76
KWHERE = ((Y0, 0), (Y0, 256), (Z0, 0), (X0, 0))
DOWN = (
    tuple(X0 + 20 + e for e in range(7)) + tuple(W0 + e for e in range(3)),
    tuple(W0 + 3 + e for e in range(6)) + tuple(Y0 + e for e in range(4)),
    tuple(Y0 + 4 + e for e in range(10)),
)

NT = (((1,), (1,)), ((), ()))
NN = (((1,), (0,)), ((), ()))


def dot(lhs, rhs, dims=NN):
    return lax.dot_general(lhs, rhs, dims, preferred_element_type=jnp.float32)


def dot_wide(lhs, rhs, dims=NN, copies=2):
    rows = lhs.shape[0]
    return dot(jnp.concatenate([lhs] * copies, axis=0), rhs, dims)[:rows]


def rms_norm(rows_f, gain):
    inv_rms = lax.rsqrt(jnp.mean(rows_f * rows_f, axis=-1, keepdims=True) + NORM_EPS)
    return (rows_f * inv_rms * gain).astype(jnp.bfloat16)


def layer_kernel(
    tok_a, exp_a, slot_a, gate_a, tok_b, exp_b, slot_b, gate_b, again_h, mgain_h, wq, wk, wv, wo, wg, wu, wd,
    out_h,
    x_v, exp_v, slot_v, gate_v, again, mgain, pool, qkv, ctx, u_all, codes, gts, disp, comb_t, xg, hid, o_v,
    p_send, p_recv, s_send, r_recv, keep, acc,
    in_sem, q_sem, o_sem, g_sem, d_sem, c_send, c_recv, u_send, u_recv, ps_sem, pr_sem, ss_sem, rr_sem,
):
    me = lax.axis_index("ep")
    dp = lax.axis_index("dp")
    x_pos = me // 2
    core = lax.rem(me, 2)
    sib = (dp, x_pos * 2 + (1 - core))
    cross = (dp, (1 - x_pos) * 2 + core)

    ins = []
    for i, (src, dst) in enumerate([
        (tok_a, x_v.at[pl.ds(0, SEQ)]), (tok_b, x_v.at[pl.ds(SEQ, SEQ)]), (again_h, again),
        (exp_a, exp_v.at[0]), (exp_b, exp_v.at[1]), (slot_a, slot_v.at[0]), (slot_b, slot_v.at[1]),
        (gate_a, gate_v.at[0]), (gate_b, gate_v.at[1]), (mgain_h, mgain),
    ]):
        cp = pltpu.make_async_copy(src, dst, in_sem.at[i])
        cp.start()
        ins.append(cp)

    q_cp = []
    for i, (w, first, last) in enumerate(((wq, 0, 1), (wq, 1, 3), (wk, 0, 3), (wv, 0, 3))):
        base = X0 + (0, 0, 3, 6)[i] + first
        q_cp.append([
            pltpu.make_async_copy(w.at[pl.ds(first, last - first), :, pl.ds(c * BLK, BLK)], pool.at[pl.ds(base + 9 * c, last - first)], q_sem.at[i, c])
            for c in range(PIECES)
        ])
        for cp in q_cp[i]:
            cp.start(priority=1)
    o_cp = [pltpu.make_async_copy(wo.at[:, :, pl.ds(c * BLK, BLK)], pool.at[pl.ds(W0 + 3 * c, 3)], o_sem.at[c]) for c in range(PIECES)]
    for cp in o_cp:
        cp.start(priority=1)

    g_cp = []
    for k, (off, size) in enumerate(zip(KOFF, KS)):
        base, row = KWHERE[k]
        half = LOCAL // 2
        for j in range(2):
            g_cp.append([
                pltpu.make_async_copy(
                    w.at[pl.ds(j * half, half), pl.ds(off, size), :], pool.at[pl.ds(base + LOCAL * i + j * half, half), pl.ds(row, size), :], g_sem.at[i, 2 * k + j]
                )
                for i, w in enumerate((wg, wu))
            ])

    def fetch(k):
        for cp in (*g_cp[2 * k], *g_cp[2 * k + 1]):
            cp.start(priority=1)

    d_cp = []
    half = BLK // 2
    for p, (first, last), off, size in (
        (0, (0, 7), 0, half), (0, (7, 10), 0, half), (0, (0, 7), half, half), (0, (7, 10), half, half),
        (1, (0, 6), 0, BLK), (1, (6, 10), 0, BLK), (2, (0, 10), 0, BLK),
    ):
        src = wd.at[pl.ds(first, last - first), :, pl.ds(p * BLK + off, size)]
        dst = pool.at[pl.ds(DOWN[p][first], last - first), :, pl.ds(off, size)]
        d_cp.append(pltpu.make_async_copy(src, dst, d_sem.at[len(d_cp)]))

    barrier = pltpu.get_barrier_semaphore()
    for peer in (sib, cross):
        pl.semaphore_signal(barrier, inc=1, device_id=peer, device_id_type=MESH)

    for cp in ins:
        cp.wait()

    for b in range(2):
        s = slot_v[b]
        codes[0, b] = jnp.where(s >= 0, exp_v[b] * SLOTS + s, -1)
        gts[0, b] = gate_v[b].astype(jnp.float32)

    def remote(src, dst, ssem, rsem, dev):
        return pltpu.make_async_remote_copy(src_ref=src, dst_ref=dst, send_sem=ssem, recv_sem=rsem, device_id=dev, device_id_type=MESH)

    def exchange(buf, ssem, rsem):
        to_cross = remote(buf.at[0], buf.at[1], ssem.at[0], rsem.at[0], cross)
        to_sib = remote(buf.at[0], buf.at[2], ssem.at[1], rsem.at[1], sib)
        relay = remote(buf.at[1], buf.at[3], ssem.at[2], rsem.at[2], sib)
        return to_cross, to_sib, relay

    x_f = x_v[...].astype(jnp.float32)
    normed = rms_norm(x_f, again[...].astype(jnp.float32).reshape(1, DIM))

    def project(first, last):
        for i in range(first, last):
            res = sum(dot_wide(normed[:, c * BLK:(c + 1) * BLK], pool[X0 + 9 * c + i], NT, 4) for c in range(PIECES))
            qkv[i] = res.astype(jnp.bfloat16)

    def arrived(copies):
        for cp in copies:
            cp.wait()

    arrived(q_cp[0])
    fetch(0)
    project(0, 1)
    arrived(q_cp[1])
    fetch(1)
    project(1, 3)

    arrived(q_cp[2])
    fetch(2)
    project(3, 6)

    pl.semaphore_wait(barrier, 2)
    c_copies = exchange(codes, c_send.at[0], c_recv.at[0])
    g_copies = exchange(gts, c_send.at[1], c_recv.at[1])
    for cp in (*c_copies[:2], *g_copies[:2]):
        cp.start()

    arrived(q_cp[3])
    q_row = lax.rem(lax.broadcasted_iota(jnp.int32, (4 * ROWS, ROWS), 0), ROWS)
    k_col = lax.broadcasted_iota(jnp.int32, (4 * ROWS, ROWS), 1)
    seen = (k_col <= q_row) & (k_col // SEQ == q_row // SEQ)
    lane_head = lax.broadcasted_iota(jnp.int32, (ROWS, 4 * HEAD), 1) // HEAD
    groups = QCH // 256
    probs = []
    for g in range(DIM // 256):
        part = pl.ds((g % groups) * 256, 256)
        q4 = qkv[g // groups, :, part]
        k4 = qkv[PER + g // groups, :, part]
        zero = jnp.zeros_like(q4)
        q_blocks = jnp.concatenate([jnp.where(lane_head == h, q4, zero) for h in range(4)], axis=0)
        s = dot(q_blocks, k4, NT) * (HEAD ** -0.5)
        s = jnp.where(seen, s, MASK_VALUE)
        ex = jnp.exp(s - jnp.max(s, axis=-1, keepdims=True))
        probs.append((ex / jnp.sum(ex, axis=-1, keepdims=True)).astype(jnp.bfloat16))
    project(6, 9)
    fetch(3)
    arrived(o_cp)
    for g in range(DIM // 256):
        v4 = qkv[2 * PER + g // groups, :, pl.ds((g % groups) * 256, 256)]
        mixed = dot(probs[g], v4)
        c4 = mixed[0:ROWS]
        for h in range(1, 4):
            c4 = jnp.where(lane_head == h, mixed[h * ROWS:(h + 1) * ROWS], c4)
        ctx[:, pl.ds(g * 256, 256)] = c4.astype(jnp.bfloat16)

    mixed_in = ctx[...]
    attn_out = [sum(dot_wide(mixed_in[:, i * BLK:(i + 1) * BLK], pool[W0 + 3 * c + i]) for i in range(3)) for c in range(PIECES)]
    h = (x_f + jnp.concatenate(attn_out, axis=1)).astype(jnp.bfloat16)
    keep[...] = h.astype(jnp.float32)
    u_all[0] = rms_norm(h.astype(jnp.float32), mgain[...].astype(jnp.float32).reshape(1, DIM))

    u_copies = []
    for k, (off, size) in enumerate(zip(KOFF, KS)):
        view = u_all.at[:, :, pl.ds(off, size)]
        u_copies.append(exchange(view, u_send.at[k], u_recv.at[k]))
        u_copies[k][0].start()
    for copies in u_copies:
        copies[1].start()

    for cp in d_cp[:5]:
        cp.start(priority=1)

    c_copies[0].wait_recv()
    c_copies[2].start()
    g_copies[0].wait_recv()
    g_copies[2].start()
    for cp in (c_copies[1], g_copies[1], c_copies[2], g_copies[2]):
        cp.wait_recv()
    row = lax.broadcasted_iota(jnp.int32, (RROWS, ROWS), 0)
    want = (row // (2 * SLOTS) + me * LOCAL) * SLOTS + lax.rem(row, SLOTS) + lax.rem(row // SLOTS, 2) * (EXPERTS * SLOTS)
    for r in range(GROUP):
        code = jnp.concatenate([codes[r, 0], jnp.where(codes[r, 1] >= 0, codes[r, 1] + EXPERTS * SLOTS, -1)], axis=1)
        gate = jnp.concatenate([gts[r, 0], gts[r, 1]], axis=1)
        val = jnp.zeros((RROWS, ROWS), jnp.float32)
        hit = jnp.zeros((RROWS, ROWS), jnp.float32)
        for j in range(TOP_K):
            same = jnp.broadcast_to(code[j:j + 1, :], (RROWS, ROWS)) == want
            val = jnp.where(same, jnp.broadcast_to(gate[j:j + 1, :], (RROWS, ROWS)), val)
            hit = jnp.where(same, 1.0, hit)
        disp[r] = hit.astype(jnp.bfloat16)
        comb_t[r] = val.T.astype(jnp.bfloat16)

    def gather(r, k):
        ks = pl.ds(KOFF[k], KS[k])
        xg[r, :, :, ks] = dot(disp[r], u_all[r, :, ks]).astype(jnp.bfloat16).reshape(LOCAL, 2 * SLOTS, KS[k])

    for k in range(len(KS)):
        gather(0, k)
    for k in range(len(KS)):
        u_copies[k][1].wait_recv()
    for k in range(len(KS)):
        gather(2, k)

    def relay(k):
        u_copies[k][0].wait_recv()
        u_copies[k][2].start()

    def experts(k, first, last):
        ks = pl.ds(KOFF[k], KS[k])
        for e in range(first, last):
            xe = xg[:, e, :, ks].reshape(EROWS, KS[k])
            base, row = KWHERE[k]
            rows = pl.ds(row, KS[k])
            gate_act = dot_wide(xe, pool[base + e, rows, :])
            up_act = dot_wide(xe, pool[base + LOCAL + e, rows, :])
            if k > 0:
                gate_act = acc[e, 0] + gate_act
                up_act = acc[e, 1] + up_act
            if k + 1 < len(KS):
                acc[e, 0] = gate_act
                acc[e, 1] = up_act
            else:
                hid[:, e] = (jax.nn.silu(gate_act) * up_act).astype(jnp.bfloat16).reshape(GROUP, 2 * SLOTS, FFN)

    relay(0)
    gather(1, 0)
    relay(1)
    gather(1, 1)
    for k in range(len(KS)):
        if k == 1:
            relay(2)
            gather(1, 2)
        u_copies[k][2].wait_recv()
        arrived(g_cp[2 * k])
        if k < 3:
            arrived(g_cp[2 * k + 1])
        gather(3, k)
        half = LOCAL // 2
        experts(k, 0, half)
        if k == 2:
            relay(3)
            gather(1, 3)
        if k == 3:
            arrived(g_cp[2 * k + 1])
        experts(k, half, LOCAL)
        if k == 1:
            for cp in d_cp[5:]:
                cp.start(priority=1)

    cols = [pl.ds(NOFF[n], NBS[n]) for n in range(NBLK)]
    to_sib = [[remote(p_send.at[i, :, c], p_recv.at[i, :, c], ps_sem.at[n, i], pr_sem.at[n, i], sib) for i in range(2)] for n, c in enumerate(cols)]
    to_cross = [remote(s_send.at[:, c], r_recv.at[:, c], ss_sem.at[n], rr_sem.at[n], cross) for n, c in enumerate(cols)]

    def forward(n):
        to_sib[n][1].wait_recv()
        s_send[:, cols[n]] = s_send[:, cols[n]] + p_recv[1, :, cols[n]]
        to_cross[n].start()

    def down(n):
        p, off = NOFF[n] // BLK, NOFF[n] % BLK
        for e in range(LOCAL):
            res = dot_wide(hid[:, e].reshape(EROWS, FFN), pool[DOWN[p][e], :, pl.ds(off, NBS[n])])
            o_v[n % 2, :, e, :, pl.ds(0, NBS[n])] = res.astype(jnp.bfloat16).reshape(GROUP, 2 * SLOTS, NBS[n])

    def combine(n, r):
        return dot(comb_t[r], o_v[n % 2, r, :, :, pl.ds(0, NBS[n])].reshape(RROWS, NBS[n]))

    arrived(d_cp[:2])
    down(0)
    p_send[1, :, cols[0]] = combine(0, 3)
    to_sib[0][1].start()
    for n in range(NBLK):
        if n == 0:
            arrived(d_cp[2:4])
        if n + 1 < NBLK and NOFF[n + 1] == BLK:
            arrived(d_cp[4:6])
        if n + 1 < NBLK and NOFF[n + 1] == 2 * BLK:
            arrived(d_cp[6:])
        if n > 0:
            p_send[1, :, cols[n]] = combine(n, 3)
        s_send[:, cols[n]] = combine(n, 1)
        p_send[0, :, cols[n]] = combine(n, 2)
        keep[:, cols[n]] = keep[:, cols[n]] + combine(n, 0)
        if n + 1 < NBLK:
            down(n + 1)
        if n > 0:
            to_sib[n][1].start()
        to_sib[n][0].start()
        if n > 1:
            forward(n - 1)
        if n == 0:
            forward(0)
    forward(NBLK - 1)

    for n in range(NBLK):
        to_sib[n][0].wait_recv()
        to_cross[n].wait_recv()
        out_h[:, cols[n]] = (keep[:, cols[n]] + p_recv[0, :, cols[n]] + r_recv[:, cols[n]]).astype(jnp.bfloat16)

    for cp in (*c_copies, *g_copies, *(c for cs in u_copies for c in cs), *(c for cs in to_sib for c in cs), *to_cross):
        cp.wait_send()


def device_fn(tokens_a, experts_a, slots_a, gates_a, tokens_b, experts_b, slots_b, gates_b, attn_gain, w_query, w_key, w_value, w_out, moe_gain, w_gate, w_up, w_down):
    def by_row(w):
        return jnp.transpose(w, (1, 2, 0)).reshape(3, BLK, DIM)

    operands = (
        tokens_a, experts_a.T, slots_a.T, gates_a.T, tokens_b, experts_b.T, slots_b.T, gates_b.T, attn_gain, moe_gain,
        by_row(w_query), by_row(w_key), by_row(w_value), w_out.reshape(3, BLK, DIM), w_gate, w_up, w_down,
    )
    operands = tuple(pltpu.with_memory_space_constraint(x, pltpu.HBM) for x in operands)
    bf16, f32, i32 = jnp.bfloat16, jnp.float32, jnp.int32
    dma = pltpu.SemaphoreType.DMA
    scratch = [
        pltpu.VMEM((ROWS, DIM), bf16), pltpu.VMEM((2, TOP_K, SEQ), i32), pltpu.VMEM((2, TOP_K, SEQ), i32), pltpu.VMEM((2, TOP_K, SEQ), bf16),
        pltpu.VMEM((DIM,), bf16), pltpu.VMEM((DIM,), bf16),
        pltpu.VMEM((POOL, BLK, BLK), bf16),
        pltpu.VMEM((NQ, ROWS, QCH), bf16), pltpu.VMEM((ROWS, DIM), bf16), pltpu.VMEM((GROUP, ROWS, DIM), bf16),
        pltpu.VMEM((GROUP, 2, TOP_K, SEQ), i32), pltpu.VMEM((GROUP, 2, TOP_K, SEQ), f32),
        pltpu.VMEM((GROUP, RROWS, ROWS), bf16), pltpu.VMEM((GROUP, ROWS, RROWS), bf16),
        pltpu.VMEM((GROUP, LOCAL, 2 * SLOTS, DIM), bf16), pltpu.VMEM((GROUP, LOCAL, 2 * SLOTS, FFN), bf16), pltpu.VMEM((2, GROUP, LOCAL, 2 * SLOTS, max(NBS)), bf16),
        pltpu.VMEM((2, ROWS, DIM), f32), pltpu.VMEM((2, ROWS, DIM), f32), pltpu.VMEM((ROWS, DIM), f32), pltpu.VMEM((ROWS, DIM), f32),
        pltpu.VMEM((ROWS, DIM), f32), pltpu.VMEM((LOCAL, 2, EROWS, FFN), f32),
        dma((10,)), dma((4, PIECES)), dma((PIECES,)), dma((2, 2 * len(KS))), dma((7,)),
        dma((2, 3)), dma((2, 3)), dma((len(KS), 3)), dma((len(KS), 3)), dma((NBLK, 2)), dma((NBLK, 2)), dma((NBLK,)), dma((NBLK,)),
    ]
    both = pl.pallas_call(
        layer_kernel,
        out_shape=jax.ShapeDtypeStruct((ROWS, DIM), bf16),
        in_specs=[pl.BlockSpec(memory_space=pltpu.HBM)] * len(operands),
        out_specs=pl.BlockSpec(memory_space=pltpu.VMEM),
        scratch_shapes=scratch,
        compiler_params=pltpu.CompilerParams(collective_id=0, has_side_effects=True, vmem_limit_bytes=VMEM_LIMIT),
        name="moe_layer",
    )(*operands)
    return split(both)


def split_kernel(both, out_a, out_b, sem):
    copies = [pltpu.make_async_copy(both.at[pl.ds(i * SEQ, SEQ)], dst, sem.at[i]) for i, dst in enumerate((out_a, out_b))]
    for cp in copies:
        cp.start()
    for cp in copies:
        cp.wait()


def split(both):
    shape = jax.ShapeDtypeStruct((SEQ, DIM), jnp.bfloat16)
    return pl.pallas_call(
        split_kernel,
        out_shape=(shape, shape),
        in_specs=[pl.BlockSpec(memory_space=pl.ANY)],
        out_specs=[pl.BlockSpec(memory_space=pl.ANY)] * 2,
        scratch_shapes=[pltpu.SemaphoreType.DMA((2,))],
        compiler_params=pltpu.CompilerParams(vmem_limit_bytes=1 << 20),
        name="split",
    )(both)


def solution(mesh):
    row_spec = P(("dp", "ep"), None)
    full_spec = P(None, None, None)
    gain_spec = P(None)
    expert_spec = P("ep", None, None)
    in_specs = (row_spec, row_spec, row_spec, row_spec, row_spec, row_spec, row_spec, row_spec, gain_spec, full_spec, full_spec, full_spec, full_spec, gain_spec, expert_spec, expert_spec, expert_spec)
    return jax.shard_map(device_fn, mesh=mesh, in_specs=in_specs, out_specs=(row_spec, row_spec), check_vma=False)
```

```python
import functools

import jax
import jax.numpy as jnp
from jax import lax
from jax.experimental import pallas as pl
from jax.experimental.pallas import tpu as pltpu
from jax.sharding import PartitionSpec as P

NORM_EPS = 1e-6
MASK_VALUE = -1e30
MESH = pl.DeviceIdType.MESH
VMEM_LIMIT = 53_000_000

SEQ = 32
ROWS = 2 * SEQ
TOP_K = 8
DIM = 1536
HEAD = 64
FFN = 512
SLOTS = 8
LOCAL = 10
EXPERTS = 40
GROUP = 4
TOKENS = GROUP * ROWS
EROWS = GROUP * 2 * SLOTS
RROWS = LOCAL * 2 * SLOTS
KS = (256, 256, 512, 512)
KOFF = tuple(sum(KS[:k]) for k in range(len(KS)))
NBS = (256, 256, 256, 256, 256, 256)
NOFF = tuple(sum(NBS[:n]) for n in range(len(NBS)))
NBLK = len(NBS)
QCH = 512
PER = DIM // QCH
NQ = 3 * PER

BLK = 512
PIECES = DIM // BLK
X0, W0, Y0, Z0 = 0, 27, 36, 56
POOL = 76
KPARTS = (((0, 10),), ((0, 10),), ((0, 5), (5, 10)), ((0, 5), (5, 8), (8, 10)))
KWHERE = ((Y0, 0), (Y0, 256), (Z0, 0), (X0, 0))
DOWN = (
    tuple(X0 + 20 + e for e in range(7)) + tuple(W0 + e for e in range(3)),
    tuple(W0 + 3 + e for e in range(6)) + tuple(Y0 + e for e in range(4)),
    tuple(Y0 + 4 + e for e in range(10)),
)

NT = (((1,), (1,)), ((), ()))
NN = (((1,), (0,)), ((), ()))


def dot(lhs, rhs, dims=NN):
    return lax.dot_general(lhs, rhs, dims, preferred_element_type=jnp.float32)


def dot_wide(lhs, rhs, dims=NN, copies=2):
    rows = lhs.shape[0]
    return dot(jnp.concatenate([lhs] * copies, axis=0), rhs, dims)[:rows]


def rms_norm(rows_f, gain):
    inv_rms = lax.rsqrt(jnp.mean(rows_f * rows_f, axis=-1, keepdims=True) + NORM_EPS)
    return (rows_f * inv_rms * gain).astype(jnp.bfloat16)


def layer_kernel(
    tok_a, exp_a, slot_a, gate_a, tok_b, exp_b, slot_b, gate_b, again_h, mgain_h, wq, wk, wv, wo, wg, wu, wd,
    out_h,
    x_v, exp_v, slot_v, gate_v, again, mgain, pool, qkv, ctx, u_all, codes, gts, disp, comb_t, xg, hid, o_v,
    p_send, p_recv, s_send, r_recv, keep, acc,
    in_sem, q_sem, o_sem, g_sem, c_send, c_recv, u_send, u_recv, ps_sem, pr_sem, ss_sem, rr_sem,
):
    me = lax.axis_index("ep")
    dp = lax.axis_index("dp")
    x_pos = me // 2
    core = lax.rem(me, 2)
    sib = (dp, x_pos * 2 + (1 - core))
    cross = (dp, (1 - x_pos) * 2 + core)
    diag = (dp, (1 - x_pos) * 2 + (1 - core))

    ins = []
    for i, (src, dst) in enumerate([
        (tok_a, x_v.at[pl.ds(0, SEQ)]), (tok_b, x_v.at[pl.ds(SEQ, SEQ)]), (again_h, again),
        (exp_a, exp_v.at[0]), (exp_b, exp_v.at[1]), (slot_a, slot_v.at[0]), (slot_b, slot_v.at[1]),
        (gate_a, gate_v.at[0]), (gate_b, gate_v.at[1]), (mgain_h, mgain),
    ]):
        cp = pltpu.make_async_copy(src, dst, in_sem.at[i])
        cp.start()
        ins.append(cp)

    q_cp = []
    for i, (w, first, last) in enumerate(((wq, 0, 1), (wq, 1, 3), (wk, 0, 3), (wv, 0, 3))):
        base = X0 + (0, 0, 3, 6)[i] + first
        q_cp.append([
            pltpu.make_async_copy(w.at[pl.ds(first, last - first), :, pl.ds(c * BLK, BLK)], pool.at[pl.ds(base + 9 * c, last - first)], q_sem.at[i, c])
            for c in range(PIECES)
        ])
        for cp in q_cp[i]:
            cp.start(priority=1)
    o_cp = [pltpu.make_async_copy(wo.at[:, :, pl.ds(c * BLK, BLK)], pool.at[pl.ds(W0 + 3 * c, 3)], o_sem.at[c]) for c in range(PIECES)]
    for cp in o_cp:
        cp.start(priority=1)

    def part_sem(k, j, i):
        if k < 2:
            return g_sem.at[i, k]
        at = 2 * j + i + (4 if k == 3 else 0)
        return q_sem.at[at // PIECES, at % PIECES]

    g_cp = []
    for k, (off, size) in enumerate(zip(KOFF, KS)):
        base, row = KWHERE[k]
        g_cp.append([])
        for j, (first, last) in enumerate(KPARTS[k]):
            ex = pl.ds(first, last - first)
            g_cp[k].append([
                pltpu.make_async_copy(w.at[ex, pl.ds(off, size), :], pool.at[pl.ds(base + LOCAL * i + first, last - first), pl.ds(row, size), :], part_sem(k, j, i))
                for i, w in enumerate((wg, wu))
            ])

    def fetch(k):
        for part in g_cp[k]:
            for cp in part:
                cp.start(priority=1)

    d_cp = []
    half = BLK // 2
    for p, (first, last), off, size in (
        (0, (0, 7), 0, half), (0, (7, 10), 0, half), (0, (0, 7), half, half), (0, (7, 10), half, half),
        (1, (0, 6), 0, BLK), (1, (6, 10), 0, BLK), (2, (0, 10), 0, BLK),
    ):
        src = wd.at[pl.ds(first, last - first), :, pl.ds(p * BLK + off, size)]
        dst = pool.at[pl.ds(DOWN[p][first], last - first), :, pl.ds(off, size)]
        d_cp.append(pltpu.make_async_copy(src, dst, in_sem.at[len(d_cp)]))

    barrier = pltpu.get_barrier_semaphore()
    for peer in (sib, cross, diag):
        pl.semaphore_signal(barrier, inc=1, device_id=peer, device_id_type=MESH)

    for cp in ins:
        cp.wait()

    for b in range(2):
        s = slot_v[b]
        codes[0, b] = jnp.where(s >= 0, exp_v[b] * SLOTS + s, -1)
        gts[0, b] = gate_v[b].astype(jnp.float32)

    def remote(src, dst, ssem, rsem, dev):
        return pltpu.make_async_remote_copy(src_ref=src, dst_ref=dst, send_sem=ssem, recv_sem=rsem, device_id=dev, device_id_type=MESH)

    def exchange(buf, ssem, rsem):
        to_cross = remote(buf.at[0], buf.at[1], ssem.at[0], rsem.at[0], cross)
        relay = remote(buf.at[1], buf.at[3], ssem.at[1], rsem.at[1], sib)
        return to_cross, relay

    x_f = x_v[...].astype(jnp.float32)
    normed = rms_norm(x_f, again[...].astype(jnp.float32).reshape(1, DIM))

    def project(first, last):
        for i in range(first, last):
            res = sum(dot_wide(normed[:, c * BLK:(c + 1) * BLK], pool[X0 + 9 * c + i], NT, 4) for c in range(PIECES))
            qkv[i] = res.astype(jnp.bfloat16)

    def arrived(copies):
        for cp in copies:
            cp.wait()

    arrived(q_cp[0])
    fetch(0)
    project(0, 1)
    arrived(q_cp[1])
    fetch(1)
    project(1, 3)

    arrived(q_cp[2])
    fetch(2)
    project(3, 6)

    pl.semaphore_wait(barrier, 3)
    c_copies = [
        remote(buf.at[0], buf.at[r], c_send.at[i, r - 1], c_recv.at[i, r - 1], dev)
        for i, buf in enumerate((codes, gts)) for r, dev in ((1, cross), (2, sib), (3, diag))
    ]
    for cp in c_copies:
        cp.start()

    arrived(q_cp[3])
    q_row = lax.rem(lax.broadcasted_iota(jnp.int32, (4 * ROWS, ROWS), 0), ROWS)
    k_col = lax.broadcasted_iota(jnp.int32, (4 * ROWS, ROWS), 1)
    seen = (k_col <= q_row) & (k_col // SEQ == q_row // SEQ)
    lane_head = lax.broadcasted_iota(jnp.int32, (ROWS, 4 * HEAD), 1) // HEAD
    groups = QCH // 256
    probs = []
    for g in range(DIM // 256):
        part = pl.ds((g % groups) * 256, 256)
        q4 = qkv[g // groups, :, part]
        k4 = qkv[PER + g // groups, :, part]
        zero = jnp.zeros_like(q4)
        q_blocks = jnp.concatenate([jnp.where(lane_head == h, q4, zero) for h in range(4)], axis=0)
        s = dot(q_blocks, k4, NT) * (HEAD ** -0.5)
        s = jnp.where(seen, s, MASK_VALUE)
        ex = jnp.exp(s - jnp.max(s, axis=-1, keepdims=True))
        probs.append((ex / jnp.sum(ex, axis=-1, keepdims=True)).astype(jnp.bfloat16))
    project(6, 9)
    fetch(3)
    arrived(o_cp)
    for g in range(DIM // 256):
        v4 = qkv[2 * PER + g // groups, :, pl.ds((g % groups) * 256, 256)]
        mixed = dot(probs[g], v4)
        c4 = mixed[0:ROWS]
        for h in range(1, 4):
            c4 = jnp.where(lane_head == h, mixed[h * ROWS:(h + 1) * ROWS], c4)
        ctx[:, pl.ds(g * 256, 256)] = c4.astype(jnp.bfloat16)

    mixed_in = ctx[...]
    attn_out = [sum(dot_wide(mixed_in[:, i * BLK:(i + 1) * BLK], pool[W0 + 3 * c + i]) for i in range(3)) for c in range(PIECES)]
    h = (x_f + jnp.concatenate(attn_out, axis=1)).astype(jnp.bfloat16)
    keep[...] = h.astype(jnp.float32)
    u_all[0] = rms_norm(h.astype(jnp.float32), mgain[...].astype(jnp.float32).reshape(1, DIM))

    u_copies = []
    for k, (off, size) in enumerate(zip(KOFF, KS)):
        view = u_all.at[:, :, pl.ds(off, size)]
        u_copies.append(exchange(view, u_send.at[k], u_recv.at[k]))
        u_copies[k][0].start()
    u_sib = remote(u_all.at[0], u_all.at[2], u_send.at[len(KS), 0], u_recv.at[len(KS), 0], sib)
    u_sib.start()

    for cp in d_cp[:5]:
        cp.start(priority=1)

    for cp in c_copies:
        cp.wait_recv()
    row = lax.broadcasted_iota(jnp.int32, (RROWS, ROWS), 0)
    want = (row // (2 * SLOTS) + me * LOCAL) * SLOTS + lax.rem(row, SLOTS) + lax.rem(row // SLOTS, 2) * (EXPERTS * SLOTS)
    for r in range(GROUP):
        code = jnp.concatenate([codes[r, 0], jnp.where(codes[r, 1] >= 0, codes[r, 1] + EXPERTS * SLOTS, -1)], axis=1)
        gate = jnp.concatenate([gts[r, 0], gts[r, 1]], axis=1)
        val = jnp.zeros((RROWS, ROWS), jnp.float32)
        hit = jnp.zeros((RROWS, ROWS), jnp.float32)
        for j in range(TOP_K):
            same = jnp.broadcast_to(code[j:j + 1, :], (RROWS, ROWS)) == want
            val = jnp.where(same, jnp.broadcast_to(gate[j:j + 1, :], (RROWS, ROWS)), val)
            hit = jnp.where(same, 1.0, hit)
        disp[r] = hit.astype(jnp.bfloat16)
        comb_t[r] = val.T.astype(jnp.bfloat16)

    def gather(r, k):
        ks = pl.ds(KOFF[k], KS[k])
        xg[r, :, :, ks] = dot(disp[r], u_all[r, :, ks]).astype(jnp.bfloat16).reshape(LOCAL, 2 * SLOTS, KS[k])

    def relay(k):
        u_copies[k][0].wait_recv()
        u_copies[k][1].start()

    def experts(k, first, last):
        ks = pl.ds(KOFF[k], KS[k])
        for e in range(first, last):
            xe = xg[:, e, :, ks].reshape(EROWS, KS[k])
            base, row = KWHERE[k]
            rows = pl.ds(row, KS[k])
            gate_act = dot_wide(xe, pool[base + e, rows, :])
            up_act = dot_wide(xe, pool[base + LOCAL + e, rows, :])
            if k > 0:
                gate_act = acc[e, 0] + gate_act
                up_act = acc[e, 1] + up_act
            if k + 1 < len(KS):
                acc[e, 0] = gate_act
                acc[e, 1] = up_act
            else:
                hid[:, e] = (jax.nn.silu(gate_act) * up_act).astype(jnp.bfloat16).reshape(GROUP, 2 * SLOTS, FFN)

    relay(0)
    for k in range(len(KS)):
        gather(0, k)
    relay(1)
    u_sib.wait_recv()
    for k in range(len(KS)):
        gather(2, k)
    gather(1, 0)
    gather(1, 1)
    for k in range(len(KS)):
        if k == 1:
            relay(2)
            gather(1, 2)
        u_copies[k][1].wait_recv()
        arrived(g_cp[k][0])
        gather(3, k)
        if k == 2:
            experts(k, 0, 5)
            relay(3)
            gather(1, 3)
            arrived(g_cp[k][1])
            experts(k, 5, LOCAL)
        else:
            for part, (first, last) in zip(g_cp[k], KPARTS[k]):
                if first > 0:
                    arrived(part)
                experts(k, first, last)
        if k == 1:
            for cp in d_cp[5:]:
                cp.start(priority=1)

    cols = [pl.ds(NOFF[n], NBS[n]) for n in range(NBLK)]
    to_sib = [[remote(p_send.at[i, :, c], p_recv.at[i, :, c], ps_sem.at[n, i], pr_sem.at[n, i], sib) for i in range(2)] for n, c in enumerate(cols)]
    to_cross = [remote(s_send.at[:, c], r_recv.at[:, c], ss_sem.at[n], rr_sem.at[n], cross) for n, c in enumerate(cols)]

    def forward(n):
        to_sib[n][1].wait_recv()
        s_send[:, cols[n]] = s_send[:, cols[n]] + p_recv[1, :, cols[n]]
        to_cross[n].start()

    def down(n):
        p, off = NOFF[n] // BLK, NOFF[n] % BLK
        for e in range(LOCAL):
            res = dot_wide(hid[:, e].reshape(EROWS, FFN), pool[DOWN[p][e], :, pl.ds(off, NBS[n])])
            o_v[n % 2, :, e, :, pl.ds(0, NBS[n])] = res.astype(jnp.bfloat16).reshape(GROUP, 2 * SLOTS, NBS[n])

    def combine(n, r):
        return dot(comb_t[r], o_v[n % 2, r, :, :, pl.ds(0, NBS[n])].reshape(RROWS, NBS[n]))

    arrived(d_cp[:2])
    down(0)
    p_send[1, :, cols[0]] = combine(0, 3)
    to_sib[0][1].start()
    for n in range(NBLK):
        if n == 0:
            arrived(d_cp[2:4])
        if n + 1 < NBLK and NOFF[n + 1] == BLK:
            arrived(d_cp[4:6])
        if n + 1 < NBLK and NOFF[n + 1] == 2 * BLK:
            arrived(d_cp[6:])
        if n > 0:
            p_send[1, :, cols[n]] = combine(n, 3)
        s_send[:, cols[n]] = combine(n, 1)
        p_send[0, :, cols[n]] = combine(n, 2)
        keep[:, cols[n]] = keep[:, cols[n]] + combine(n, 0)
        if n + 1 < NBLK:
            down(n + 1)
        if n > 0:
            to_sib[n][1].start()
        to_sib[n][0].start()
        if n > 1:
            forward(n - 1)
        if n == 0:
            forward(0)
    forward(NBLK - 1)

    for n in range(NBLK):
        to_sib[n][0].wait_recv()
        to_cross[n].wait_recv()
        out_h[:, cols[n]] = (keep[:, cols[n]] + p_recv[0, :, cols[n]] + r_recv[:, cols[n]]).astype(jnp.bfloat16)

    for cp in (*c_copies, u_sib, *(c for cs in u_copies for c in cs), *(c for cs in to_sib for c in cs), *to_cross):
        cp.wait_send()


def device_fn(tokens_a, experts_a, slots_a, gates_a, tokens_b, experts_b, slots_b, gates_b, attn_gain, w_query, w_key, w_value, w_out, moe_gain, w_gate, w_up, w_down):
    def by_row(w):
        return jnp.transpose(w, (1, 2, 0)).reshape(3, BLK, DIM)

    operands = (
        tokens_a, experts_a.T, slots_a.T, gates_a.T, tokens_b, experts_b.T, slots_b.T, gates_b.T, attn_gain, moe_gain,
        by_row(w_query), by_row(w_key), by_row(w_value), w_out.reshape(3, BLK, DIM), w_gate, w_up, w_down,
    )
    operands = tuple(pltpu.with_memory_space_constraint(x, pltpu.HBM) for x in operands)
    bf16, f32, i32 = jnp.bfloat16, jnp.float32, jnp.int32
    dma = pltpu.SemaphoreType.DMA
    scratch = [
        pltpu.VMEM((ROWS, DIM), bf16), pltpu.VMEM((2, TOP_K, SEQ), i32), pltpu.VMEM((2, TOP_K, SEQ), i32), pltpu.VMEM((2, TOP_K, SEQ), bf16),
        pltpu.VMEM((DIM,), bf16), pltpu.VMEM((DIM,), bf16),
        pltpu.VMEM((POOL, BLK, BLK), bf16),
        pltpu.VMEM((NQ, ROWS, QCH), bf16), pltpu.VMEM((ROWS, DIM), bf16), pltpu.VMEM((GROUP, ROWS, DIM), bf16),
        pltpu.VMEM((GROUP, 2, TOP_K, SEQ), i32), pltpu.VMEM((GROUP, 2, TOP_K, SEQ), f32),
        pltpu.VMEM((GROUP, RROWS, ROWS), bf16), pltpu.VMEM((GROUP, ROWS, RROWS), bf16),
        pltpu.VMEM((GROUP, LOCAL, 2 * SLOTS, DIM), bf16), pltpu.VMEM((GROUP, LOCAL, 2 * SLOTS, FFN), bf16), pltpu.VMEM((2, GROUP, LOCAL, 2 * SLOTS, max(NBS)), bf16),
        pltpu.VMEM((2, ROWS, DIM), f32), pltpu.VMEM((2, ROWS, DIM), f32), pltpu.VMEM((ROWS, DIM), f32), pltpu.VMEM((ROWS, DIM), f32),
        pltpu.VMEM((ROWS, DIM), f32), pltpu.VMEM((LOCAL, 2, EROWS, FFN), f32),
        dma((10,)), dma((4, PIECES)), dma((PIECES,)), dma((2, 2)),
        dma((2, 3)), dma((2, 3)), dma((len(KS) + 1, 2)), dma((len(KS) + 1, 2)), dma((NBLK, 2)), dma((NBLK, 2)), dma((NBLK,)), dma((NBLK,)),
    ]
    both = pl.pallas_call(
        layer_kernel,
        out_shape=jax.ShapeDtypeStruct((ROWS, DIM), bf16),
        in_specs=[pl.BlockSpec(memory_space=pltpu.HBM)] * len(operands),
        out_specs=pl.BlockSpec(memory_space=pltpu.VMEM),
        scratch_shapes=scratch,
        compiler_params=pltpu.CompilerParams(collective_id=0, has_side_effects=True, vmem_limit_bytes=VMEM_LIMIT),
        name="moe_layer",
    )(*operands)
    return split(both)


def split_kernel(both, out_a, out_b, sem):
    copies = [pltpu.make_async_copy(both.at[pl.ds(i * SEQ, SEQ)], dst, sem.at[i]) for i, dst in enumerate((out_a, out_b))]
    for cp in copies:
        cp.start()
    for cp in copies:
        cp.wait()


def split(both):
    shape = jax.ShapeDtypeStruct((SEQ, DIM), jnp.bfloat16)
    return pl.pallas_call(
        split_kernel,
        out_shape=(shape, shape),
        in_specs=[pl.BlockSpec(memory_space=pl.ANY)],
        out_specs=[pl.BlockSpec(memory_space=pl.ANY)] * 2,
        scratch_shapes=[pltpu.SemaphoreType.DMA((2,))],
        compiler_params=pltpu.CompilerParams(vmem_limit_bytes=1 << 20),
        name="split",
    )(both)


def solution(mesh):
    row_spec = P(("dp", "ep"), None)
    full_spec = P(None, None, None)
    gain_spec = P(None)
    expert_spec = P("ep", None, None)
    in_specs = (row_spec, row_spec, row_spec, row_spec, row_spec, row_spec, row_spec, row_spec, gain_spec, full_spec, full_spec, full_spec, full_spec, gain_spec, expert_spec, expert_spec, expert_spec)
    return jax.shard_map(device_fn, mesh=mesh, in_specs=in_specs, out_specs=(row_spec, row_spec), check_vma=False)
```
